32 devices in a mesh: grp: 8 (over z, x), ep: 4 (over y, core).
Axes of the slice: x: 2, y: 2, z: 4, core: 2. Of those that a mesh axis runs over, the one named last changes fastest.
Arguments:
- out_grad: bfloat16 [256, 4096], P('grp', 'ep'), may hold values from -6 to 6
- expert_ids: int32 [256, 8], P('grp'), may hold values from 0 to 15, as said below
- router_logits: float32 [256, 16], P('grp'), may hold values from -5 to 5
- router_weight: bfloat16 [16, 4096], P(None, 'ep'), may hold values from -0.09375 to 0.09375
- expert_weight: bfloat16 [16, 4096, 1024], P('grp', 'ep'), may hold values from -0.1875 to 0.1875
- hidden_saved: bfloat16 [8, 512, 1024], P('grp'), may hold values from -6 to 6
Outputs:
- weight_grad: bfloat16 [16, 4096, 1024], P('grp', 'ep')
- hidden_grad: bfloat16 [8, 512, 1024], P('grp', 'ep')
- input_grad: bfloat16 [256, 4096], P('grp', 'ep')
The draws below stay inside these ranges and needn't reach their ends.
Inputs may be any that keep to these rules, and one draw needn't show every extreme that they name: `expert_ids`: each row names 8 different experts, lying in at most 4 of the 4 groups of 4 consecutive experts. In each aligned block of 32 rows no expert is named by more than 32 rows, and some expert is named by exactly 32.
All inputs are finite; a program needn't handle non-finite values.
Results may differ from the reference program's by a relative error of at most 0.02.
Values may be sent and summed in bfloat16 or wider, within the bound.
A program may use at most 64 MiB of HBM per device.

```python
import jax
import jax.numpy as jnp
from jax import lax

D = 4096
FF = 1024
EXP_GRP = 2
TOPG = 4
TOPK = 8
EXPERTS = 16
GROUPS = 4
GROUP_EXP = 4
PICK = 2
ROWS_GRP = 32
TOKENS = 256
USERS = 32
CAP = 32
SLOTS = 512
N_GRP = 8
N_EP = 4


def draw_expert_ids(key, part):
    group_scores = jax.random.randint(jax.random.fold_in(key, 101), (N_GRP, GROUPS), 0, 1 << 20) * GROUPS + jnp.arange(GROUPS, dtype=jnp.int32)[None, :]
    group_order = jnp.argsort(group_scores, axis=1).astype(jnp.int32)
    user_scores = jax.random.randint(jax.random.fold_in(key, 202), (N_GRP, GROUPS, USERS), 0, 1 << 20) * USERS + jnp.arange(USERS, dtype=jnp.int32)[None, None, :]
    user_order = jnp.argsort(user_scores, axis=2).astype(jnp.int32)
    member_scores = jax.random.randint(jax.random.fold_in(key, 303), (N_GRP, GROUPS, GROUP_EXP), 0, 1 << 20) * GROUP_EXP + jnp.arange(GROUP_EXP, dtype=jnp.int32)[None, None, :]
    member_order = jnp.argsort(member_scores, axis=2).astype(jnp.int32)
    ticket = TOPG * jnp.arange(ROWS_GRP, dtype=jnp.int32)[:, None] + jnp.arange(TOPG, dtype=jnp.int32)[None, :]
    position = ticket % GROUPS
    cycle_index = ticket // GROUPS
    blocks = jnp.arange(N_GRP, dtype=jnp.int32)[:, None, None]
    group_id = group_order[blocks, position[None, :, :]]
    user_slot = user_order[blocks, position[None, :, :], cycle_index[None, :, :]]
    pick_index = user_slot[:, :, :, None] + USERS * jnp.arange(PICK, dtype=jnp.int32)[None, None, None, :]
    member_rank = jnp.where(pick_index < CAP, 0, 1 + (pick_index - CAP) % (GROUP_EXP - 1))
    member = member_order[blocks[:, :, :, None], position[None, :, :, None], member_rank]
    experts = group_id[:, :, :, None] * GROUP_EXP + member
    return experts.reshape(TOKENS, TOPK).astype(jnp.int32)


def level_of(stream_key, extent, shards, low, top_value):
    loudness = 1.0
    for dim, blocks in shards:
        draws = jax.random.uniform(jax.random.fold_in(jax.random.fold_in(stream_key, 6), dim), (blocks,), jnp.float32, low / len(shards), top_value / len(shards))
        loudness = loudness * jnp.repeat(jnp.exp(draws), extent[dim] // blocks).reshape((-1,) + (1,) * (len(extent) - 1 - dim))
    return loudness


def bell_draw(key, shape, scale, reach, pieces=(), kind=jnp.bfloat16):
    entries = scale * jax.random.normal(key, shape, jnp.float32)
    if pieces:
        entries = entries * level_of(key, shape, pieces, -0.22, 0.18)
    return jnp.clip(entries, -reach, reach).astype(kind)


def setup_inputs(seed: int = 0) -> dict:
    key_list = jax.random.split(jax.random.key(seed), 7)
    return {
        "out_grad": bell_draw(key_list[0], (TOKENS, D), 1.0, 6.0, ((0, 8), (1, 4))),
        "expert_ids": draw_expert_ids(jax.random.fold_in(key_list[6], 71), 0),
        "router_logits": bell_draw(key_list[2], (TOKENS, EXPERTS), 1.0, 5.0, ((0, 8),), jnp.float32),
        "router_weight": bell_draw(key_list[3], (EXPERTS, D), D ** -0.5, 0.09375, ((1, 4),)),
        "expert_weight": bell_draw(key_list[4], (EXPERTS, D, FF), FF ** -0.5, 0.1875, ((0, 8), (1, 4))),
        "hidden_saved": bell_draw(key_list[5], (N_GRP, SLOTS, FF), 1.0, 6.0, ((0, 8),)),
    }


route_scale = 2.5


def slot_places(expert_ids):
    pair_rows = expert_ids.reshape(N_GRP, ROWS_GRP * TOPK)
    onehot = (pair_rows[:, :, None] == jnp.arange(EXPERTS, dtype=jnp.int32)[None, None, :]).astype(jnp.int32)
    pair_ranks = jnp.sum((jnp.cumsum(onehot, axis=1) - 1) * onehot, axis=2)
    source_block = jnp.arange(N_GRP, dtype=jnp.int32)[:, None]
    within = ((pair_rows % EXP_GRP) * N_GRP + source_block) * CAP + pair_ranks
    return ((pair_rows // EXP_GRP) * SLOTS + within).reshape(TOKENS * TOPK).astype(jnp.int32)


def reference(out_grad, expert_ids, router_logits, router_weight, expert_weight, hidden_saved):
    sig = jax.nn.sigmoid(router_logits.astype(jnp.float32))
    chosen = jnp.take_along_axis(sig, expert_ids, axis=1)
    route_probs = route_scale * chosen / jnp.sum(chosen, axis=1, keepdims=True)
    places = slot_places(expert_ids)
    pair_token = (jnp.arange(TOKENS * TOPK, dtype=jnp.int32) // TOPK).astype(jnp.int32)
    token_of_slot = jnp.zeros((N_GRP * SLOTS,), jnp.int32).at[places].set(pair_token)
    used_slot = jnp.zeros((N_GRP * SLOTS,), jnp.int32).at[places].set(jnp.ones((TOKENS * TOPK,), jnp.int32))
    slot_prob = jnp.zeros((N_GRP * SLOTS,), jnp.float32).at[places].set(route_probs.reshape(TOKENS * TOPK)).astype(jnp.bfloat16)
    span = N_GRP * CAP
    width = D // N_EP

    def owner_work(items):
        token_index, used_flag, prob_row, saved_rows, weights = items
        slot_rows = jnp.where(used_flag[:, None] > 0, out_grad[token_index], jnp.zeros((), jnp.bfloat16))
        grouped = slot_rows.reshape(EXP_GRP, span, N_EP, width).astype(jnp.float32)
        split_weights = weights.reshape(EXP_GRP, N_EP, width, FF).astype(jnp.float32)
        partial_sums = jnp.einsum("lmkd,lkdf->lkmf", grouped, split_weights)
        rounded = lax.optimization_barrier(partial_sums.astype(jnp.bfloat16)).astype(jnp.float32)
        summed = jnp.sum(rounded, axis=1).reshape(SLOTS, FF)
        prob_value = prob_row.astype(jnp.float32)
        hidden_grad = (prob_value[:, None] * summed).astype(jnp.bfloat16)
        slot_score = jnp.sum(saved_rows.astype(jnp.float32) * summed, axis=1)
        scaled_rows = (prob_value[:, None] * slot_rows.astype(jnp.float32)).astype(jnp.bfloat16)
        weight_grad = jnp.einsum(
            "lmd,lmf->ldf",
            scaled_rows.reshape(EXP_GRP, span, D).astype(jnp.float32),
            saved_rows.reshape(EXP_GRP, span, FF).astype(jnp.float32),
        ).astype(jnp.bfloat16)
        return weight_grad, hidden_grad, slot_score

    weight_grad, hidden_grad, slot_score = lax.map(
        owner_work,
        (
            token_of_slot.reshape(N_GRP, SLOTS),
            used_slot.reshape(N_GRP, SLOTS),
            slot_prob.reshape(N_GRP, SLOTS),
            hidden_saved,
            expert_weight.reshape(N_GRP, EXP_GRP, D, FF),
        ),
    )
    pair_score = slot_score.reshape(N_GRP * SLOTS)[places].reshape(TOKENS, TOPK)
    weighted_mean = jnp.sum(route_probs * pair_score, axis=1, keepdims=True) / route_scale
    logit_terms = route_probs * (1.0 - chosen) * (pair_score - weighted_mean)
    picked = expert_ids[:, :, None] == jnp.arange(EXPERTS, dtype=jnp.int32)[None, None, :]
    router_grad = jnp.sum(jnp.where(picked, logit_terms[:, :, None], jnp.zeros((), jnp.float32)), axis=1).astype(jnp.bfloat16)
    input_grad = jnp.dot(router_grad, router_weight, preferred_element_type=jnp.float32).astype(jnp.bfloat16)
    return weight_grad.reshape(EXPERTS, D, FF), hidden_grad, input_grad
```

```python
import jax
import jax.numpy as jnp
from jax import lax
from jax.experimental import pallas as pl
from jax.experimental.pallas import tpu as pltpu
from jax.sharding import PartitionSpec as P

route_scale = 2.5


def body(out_grad, expert_ids, router_logits, router_weight, expert_weight, hidden_saved):
    group_rows, features = out_grad.shape
    top_count = expert_ids.shape[1]
    experts = router_logits.shape[1]
    group_count = lax.axis_size("grp")
    local_experts = expert_weight.shape[0]
    hidden_width = expert_weight.shape[2]
    slot_count = hidden_saved.shape[1]
    capacity = slot_count // (local_experts * group_count)
    expert_span = group_count * capacity
    pair_count = group_rows * top_count
    sig_values = jax.nn.sigmoid(router_logits)
    picked = expert_ids[:, :, None] == jnp.arange(experts, dtype=jnp.int32)[None, None, :]
    chosen = jnp.sum(jnp.where(picked, sig_values[:, None, :], 0.0), axis=2)
    route_probs = route_scale * chosen / jnp.sum(chosen, axis=1, keepdims=True)
    flat_ids = expert_ids.reshape(pair_count)
    onehot = picked.reshape(pair_count, experts).astype(jnp.int32)
    pair_ranks = jnp.sum((jnp.cumsum(onehot, axis=0) - 1) * onehot, axis=1)
    slot_place = (
        flat_ids % local_experts * group_count + flat_ids // local_experts
    ) * capacity + pair_ranks
    slot_match = slot_place[None, :] == jnp.arange(slot_count, dtype=jnp.int32)[:, None]
    token_pick = jnp.sum(
        slot_match.reshape(slot_count, group_rows, top_count).astype(jnp.float32), axis=2
    ).astype(jnp.bfloat16)
    send_rows = jnp.dot(token_pick, out_grad, preferred_element_type=jnp.float32).astype(
        jnp.bfloat16
    )
    send_prob = jnp.sum(
        jnp.where(slot_match, route_probs.reshape(1, pair_count), 0.0), axis=1
    ).astype(jnp.bfloat16)
    got_rows, got_prob = (
        lax.all_to_all(
            send_rows.reshape(local_experts, group_count, capacity, features),
            "grp",
            split_axis=1,
            concat_axis=1,
            tiled=True,
        ),
        lax.all_to_all(
            send_prob.reshape(local_experts, group_count, capacity),
            "grp",
            split_axis=1,
            concat_axis=1,
            tiled=True,
        ),
    )
    slot_grads = got_rows.reshape(local_experts, expert_span, features)
    prob_rows = got_prob.reshape(local_experts, expert_span).astype(jnp.float32)
    saved_rows = hidden_saved.reshape(local_experts, expert_span, hidden_width)
    scaled_rows = (prob_rows[:, :, None] * slot_grads.astype(jnp.float32)).astype(jnp.bfloat16)
    weight_grad = jnp.einsum(
        "lmd,lmf->ldf", scaled_rows, saved_rows, preferred_element_type=jnp.float32
    ).astype(jnp.bfloat16)
    owner_index = lax.axis_index("ep")
    share_rows = slot_count // lax.axis_size("ep")
    flat_prob = prob_rows.reshape(slot_count)
    flat_saved = hidden_saved.reshape(slot_count, hidden_width)
    partial_term = jnp.einsum(
        "lmd,ldf->lmf", slot_grads, expert_weight, preferred_element_type=jnp.float32
    ).reshape(slot_count, hidden_width)
    rounded_term = lax.optimization_barrier(partial_term.astype(jnp.bfloat16)).astype(jnp.float32)
    partial_score = jnp.sum(flat_saved.astype(jnp.float32) * rounded_term, axis=1)
    moved_scores = lax.all_to_all(
        partial_score.reshape(local_experts, group_count, capacity),
        "grp",
        split_axis=1,
        concat_axis=1,
        tiled=True,
    )
    returned = lax.psum(moved_scores, "ep")
    summed = lax.psum_scatter(
        partial_term.astype(jnp.bfloat16), "ep", scatter_dimension=0, tiled=True
    ).astype(jnp.float32)
    own_prob = lax.dynamic_slice_in_dim(flat_prob, owner_index * share_rows, share_rows, 0)
    hidden_grad = (own_prob[:, None] * summed).astype(jnp.bfloat16)[None]
    pair_score = jnp.sum(
        jnp.where(slot_match, returned.reshape(slot_count, 1), 0.0), axis=0
    ).reshape(group_rows, top_count)
    weighted_mean = jnp.sum(route_probs * pair_score, axis=1, keepdims=True) / route_scale
    logit_terms = route_probs * (1.0 - chosen) * (pair_score - weighted_mean)
    router_grad = jnp.sum(jnp.where(picked, logit_terms[:, :, None], 0.0), axis=1).astype(
        jnp.bfloat16
    )
    input_grad = jnp.dot(router_grad, router_weight, preferred_element_type=jnp.float32).astype(
        jnp.bfloat16
    )
    return (weight_grad, hidden_grad, input_grad)


MESH = pl.DeviceIdType.MESH


def flip(a, j):
    out, bit = a, 1
    while bit <= j:
        if j & bit:
            out = out + bit * (1 - 2 * (a // bit % 2))
        bit *= 2
    return out


def fused_kernel(
    ids_hbm, logits_hbm, grad_hbm, rw_hbm, w_hbm, saved_hbm,
    weight_ref, hidden_ref, input_ref,
    ids_ref, logits_ref, rw_ref, w_ref, saved_ref, rows_all, probs_all, probs_own,
    slot_ref, saved_tok, scaled, part, recv_a, total_own, send_b, recv_b,
    score_own, score_recv, score_rows,
    in_sem, w_sem, rows_send, rows_recv, probs_send, probs_recv,
    a_send, a_recv, b_send, b_recv, sc_send, sc_recv,
):
    groups = lax.axis_size("grp")
    parts = lax.axis_size("ep")
    chips = parts // 2
    g = lax.axis_index("grp")
    k = lax.axis_index("ep")
    chip, core = k // 2, k % 2
    experts, rows = logits_ref.shape
    top = ids_ref.shape[0]
    _, local, _, width = part.shape
    features = rows_all.shape[1]
    half_groups = groups // 2
    half_tokens = half_groups * rows
    tokens = groups * rows
    span = saved_ref.shape[0] // local
    share = span // 2
    capacity = span // groups
    f32, bf16 = jnp.float32, jnp.bfloat16
    i32 = jnp.int32
    column, side = g // 2, lax.rem(g, 2)
    mate = g + 1 - 2 * side
    hops = list(range(half_groups - 1, 0, -1))

    barrier = pltpu.get_barrier_semaphore()
    for dg in range(groups):
        for dk in range(parts):
            if dg or dk:
                pl.semaphore_signal(
                    barrier, inc=1,
                    device_id=(lax.rem(g + dg, groups), lax.rem(k + dk, parts)),
                    device_id_type=MESH,
                )

    def block(b):
        return rows_all.at[pl.ds(pl.multiple_of(b * rows, rows), rows), :]

    fetch = [
        pltpu.make_async_copy(src, dst, in_sem.at[i])
        for i, (src, dst) in enumerate([
            (grad_hbm, block(g)), (logits_hbm, logits_ref), (ids_hbm, ids_ref),
            (saved_hbm, saved_ref), (rw_hbm, rw_ref),
        ])
    ]
    w_copies = [
        pltpu.make_async_copy(w_hbm.at[i], w_ref.at[i], w_sem.at[i]) for i in range(local)
    ]
    for copy in [*fetch[:3], *w_copies, *fetch[3:]]:
        copy.start()

    sends = []

    def go(copy, when=None):
        if when is None:
            copy.start()
            sends.append(copy.wait_send)
        else:
            pl.when(when)(copy.start)
            sends.append(lambda: pl.when(when)(copy.wait_send))

    def rows_copy(b, to, sem):
        return pltpu.make_async_remote_copy(
            src_ref=block(b), dst_ref=block(b), send_sem=rows_send.at[sem],
            recv_sem=rows_recv.at[b], device_id=(to, k), device_id_type=MESH,
        )

    def probs_copy(b, to, sem):
        return pltpu.make_async_remote_copy(
            src_ref=probs_own, dst_ref=probs_all.at[b], send_sem=probs_send.at[sem],
            recv_sem=probs_recv.at[b], device_id=(to, k), device_id_type=MESH,
        )

    fetch[0].wait()
    pl.semaphore_wait(barrier, groups * parts - 1)
    go(rows_copy(g, mate, 0))
    for j in hops:
        go(rows_copy(g, flip(column, j) * 2 + side, j))

    fetch[1].wait()
    fetch[2].wait()
    sig = 1.0 / (1.0 + jnp.exp(-logits_ref[...]))
    ids = ids_ref[...]
    expert_iota = lax.broadcasted_iota(i32, (experts, rows), 0)
    named = ids[0:1, :] == expert_iota
    for i in range(1, top):
        named = named | (ids[i : i + 1, :] == expert_iota)
    probs = route_scale * sig / jnp.sum(jnp.where(named, sig, 0.0), axis=0, keepdims=True)
    probs = jnp.where(named, probs, 0.0)
    lane_off = lax.rem(g, half_groups) * rows
    place = (
        lax.broadcasted_iota(i32, (rows, half_tokens), 1)
        == lax.broadcasted_iota(i32, (rows, half_tokens), 0) + lane_off
    )
    placed = jnp.dot(
        probs.astype(bf16), place.astype(f32).astype(bf16), preferred_element_type=f32
    ).astype(bf16)
    probs_own[...] = placed
    probs_all[g] = placed
    for j in range(1, groups):
        go(probs_copy(g, lax.rem(g + j, groups), j - 1))

    order = [lax.rem(chip + 1 + i, chips) for i in range(chips)]
    partner = k + 1 - 2 * core

    def a_copy(b):
        return pltpu.make_async_remote_copy(
            src_ref=part.at[b], dst_ref=recv_a.at[b], send_sem=a_send.at[b],
            recv_sem=a_recv.at[b], device_id=(g, partner), device_id_type=MESH,
        )

    def own(b):
        return b // half_groups == core

    def multiply(b):
        found = block(b)[...]
        for l in range(local):
            part[b, l] = jnp.dot(found, w_ref[l], preferred_element_type=f32).astype(bf16)
        go(a_copy(b), b // half_groups != core)

    def b_copy(b, l, to, source):
        at = lax.rem(b, half_groups)
        return pltpu.make_async_remote_copy(
            src_ref=send_b.at[l, at], dst_ref=recv_b.at[source, at],
            send_sem=b_send.at[l, at], recv_sem=b_recv.at[source, at],
            device_id=(g, to), device_id_type=MESH,
        )

    def finish(b):
        at = lax.rem(b, half_groups)

        @pl.when(own(b))
        def _():
            a_copy(b).wait_recv()
            for l in order[:-1]:
                both = part[b, l].astype(f32) + recv_a[b, l].astype(f32)
                send_b[l, at] = both.astype(bf16)
                b_copy(b, l, l * 2 + core, chip).start()
            total_own[at] = part[b, chip].astype(f32) + recv_a[b, chip].astype(f32)

        def end():
            for l in order[:-1]:
                b_copy(b, l, l * 2 + core, chip).wait_send()

        sends.append(lambda: pl.when(own(b))(end))

    eye = (
        lax.broadcasted_iota(i32, (rows, half_tokens), 0)
        == lax.broadcasted_iota(i32, (rows, half_tokens), 1)
    )

    def score_copy(b, to, y, o):
        return pltpu.make_async_remote_copy(
            src_ref=score_own.at[b], dst_ref=score_recv.at[y, o],
            send_sem=sc_send.at[b, to], recv_sem=sc_recv.at[y, o],
            device_id=(b, to), device_id_type=MESH,
        )

    def score(b, home=False):
        for l in range(local):
            at = pl.ds(pl.multiple_of(b * rows, rows), rows)
            value = jnp.sum(
                saved_tok[l, at, :].astype(f32) * part[b, l].astype(f32), axis=1, keepdims=True
            )
            score_own[b, l : l + 1, :] = jnp.sum(
                jnp.where(eye, value, 0.0), axis=0, keepdims=True
            )
        if home:
            score_recv[k, b] = score_own[b]
        for dk in range(1 if home else 0, parts):
            go(score_copy(b, lax.rem(k + dk, parts), k, g))

    for copy in w_copies:
        copy.wait()
    multiply(g)

    for j in range(1, groups):
        b = lax.rem(g + j, groups)
        probs_copy(b, g, 0).wait_recv()
    pick = (
        lax.broadcasted_iota(i32, (8, experts), 1)
        == lax.broadcasted_iota(i32, (8, experts), 0) + g * local
    ) & (lax.broadcasted_iota(i32, (8, experts), 0) < local)
    pick = pick.astype(f32).astype(bf16)
    lane = lax.broadcasted_iota(i32, (half_tokens, half_tokens), 1)
    line = lax.broadcasted_iota(i32, (half_tokens, half_tokens), 0)
    same = line // rows == lane // rows
    earlier = ((line < lane) & same).astype(f32).astype(bf16)
    later = ((lane < line) & same).astype(f32).astype(bf16)
    unit = (lane == line).astype(f32).astype(bf16)
    lane_block = lax.broadcasted_iota(i32, (8, half_tokens), 1) // rows
    line_block = lax.broadcasted_iota(i32, (half_tokens, 8), 0) // rows
    turn = (((1,), (1,)), ((), ()))
    fetch[3].wait()
    for h in range(2):
        total = probs_all[h * half_groups].astype(f32)
        for b in range(1, half_groups):
            total = total + probs_all[h * half_groups + b].astype(f32)
        mine = jnp.dot(pick, total.astype(bf16), preferred_element_type=f32)
        used = mine > 0.0
        marks = used.astype(f32).astype(bf16)
        rank = jnp.dot(marks, earlier, preferred_element_type=f32)
        slot = lane_block * capacity + rank.astype(i32)
        slot_ref[h, 0] = jnp.where(used, slot, -1).astype(f32)
        slot_ref[h, 1] = mine
        mine_col = lax.dot_general(unit, mine.astype(bf16), turn, preferred_element_type=f32)
        rank_col = lax.dot_general(later, marks, turn, preferred_element_type=f32)
        slot_col = jnp.where(
            mine_col > 0.0, line_block * capacity + rank_col.astype(i32), -1
        )
        spot = lax.broadcasted_iota(i32, (half_tokens, share), 1)
        at = pl.ds(h * half_tokens, half_tokens)
        for l in range(local):
            match = (slot_col[:, l : l + 1] == spot).astype(f32).astype(bf16)
            start = l * span + h * share
            saved_tok[l, at, :] = jnp.dot(
                match, saved_ref[start : start + share, :], preferred_element_type=f32
            ).astype(bf16)
            scaled[l, at, :] = jnp.broadcast_to(
                mine_col[:, l : l + 1], (half_tokens, scaled.shape[2])
            )

    rows_copy(mate, g, 0).wait_recv()
    multiply(mate)
    score(g, home=True)
    finish(g)
    score(mate)
    last = mate
    for j in hops:
        b = flip(column, j) * 2 + side
        rows_copy(b, g, 0).wait_recv()
        go(rows_copy(b, mate, half_groups + j))
        multiply(b)
        finish(last)
        score(b)
        last = b
    for j in hops:
        b = flip(column, j) * 2 + 1 - side
        rows_copy(b, g, 0).wait_recv()
        multiply(b)
        finish(last)
        score(b)
        last = b

    step = min(width, 256)
    for l in range(local):
        weighed = jnp.concatenate(
            [
                (scaled[l, :, 0:128] * rows_all[:, n : n + 128].astype(f32)).astype(bf16)
                for n in range(0, features, 128)
            ],
            axis=1,
        )
        for n in range(0, width, step):
            weight_ref[l, :, n : n + step] = lax.dot_general(
                weighed, saved_tok[l, :, n : n + step], (((0,), (0,)), ((), ())),
                preferred_element_type=f32,
            ).astype(bf16)
        if l == 0:
            finish(last)

    def pick_row(which):
        table = slot_ref[core, which]
        mask = lax.broadcasted_iota(i32, table.shape, 0) == chip
        return jnp.sum(jnp.where(mask, table, 0.0), axis=0, keepdims=True)

    spot = lax.broadcasted_iota(i32, (share, half_tokens), 0).astype(f32)
    spread = jnp.where(spot == pick_row(0), pick_row(1), 0.0).astype(bf16)
    for i in range(chips - 1):
        for at in range(half_groups):
            b_copy(at, 0, k, order[i]).wait_recv()
    total = total_own[...]
    for i in range(chips - 1):
        total = total + recv_b[order[i]].astype(f32)
    hidden_ref[...] = jnp.dot(
        spread, total.reshape(half_tokens, width).astype(bf16), preferred_element_type=f32
    ).astype(bf16)

    for y in range(parts):
        for o in range(groups):
            wait = score_copy(g, k, y, o).wait_recv
            pl.when((o != g) | (y != k))(wait)
    for o in range(groups):
        value = score_recv[0, o]
        for y in range(1, parts):
            value = value + score_recv[y, o]
        score_rows[o * local : (o + 1) * local, :] = value
    pair = score_rows[:, 0:rows]
    mean = jnp.sum(probs * pair, axis=0, keepdims=True) / route_scale
    terms = jnp.where(named, probs * (1.0 - sig) * (pair - mean), 0.0).astype(bf16)
    small = (
        lax.broadcasted_iota(i32, (rows, rows), 0) == lax.broadcasted_iota(i32, (rows, rows), 1)
    )
    turned = lax.dot_general(
        small.astype(f32).astype(bf16), terms, turn, preferred_element_type=f32
    ).astype(bf16)
    fetch[4].wait()
    input_ref[...] = jnp.dot(turned, rw_ref[...], preferred_element_type=f32).astype(bf16)

    for wait in sends:
        wait()


def write_kernel(weight_ref, hidden_ref, input_ref, weight_hbm, hidden_hbm, input_hbm, sem):
    copies = [
        pltpu.make_async_copy(hidden_ref, hidden_hbm, sem.at[0]),
        pltpu.make_async_copy(input_ref, input_hbm, sem.at[1]),
    ]
    local, features, _ = weight_ref.shape
    cut = features // 4
    for l in range(local):
        for n in range(4):
            at = pl.ds(n * cut, cut)
            copies.append(
                pltpu.make_async_copy(
                    weight_ref.at[l, at, :], weight_hbm.at[l, at, :], sem.at[2 + l * 4 + n]
                )
            )
    for copy in copies:
        copy.start()
    for copy in copies:
        copy.wait()


def fused(out_grad, expert_ids, router_logits, router_weight, expert_weight, hidden_saved):
    groups, parts = lax.axis_size("grp"), lax.axis_size("ep")
    rows, features = out_grad.shape
    experts = router_logits.shape[1]
    top = expert_ids.shape[1]
    local, _, width = expert_weight.shape
    slots = hidden_saved.shape[1]
    span = slots // local
    half_groups = groups // 2
    half_tokens = half_groups * rows
    tokens = groups * rows
    share = span // 2
    chips = parts // 2
    f32, bf16 = jnp.float32, jnp.bfloat16
    vmem = pl.BlockSpec(memory_space=pltpu.VMEM)
    hbm = pl.BlockSpec(memory_space=pltpu.HBM)
    dma = pltpu.SemaphoreType.DMA
    out_shape = (
        jax.ShapeDtypeStruct((local, features, width), bf16),
        jax.ShapeDtypeStruct((share, width), bf16),
        jax.ShapeDtypeStruct((rows, features), bf16),
    )
    outs = pl.pallas_call(
        fused_kernel,
        out_shape=out_shape,
        in_specs=[hbm] * 6,
        out_specs=(vmem, vmem, vmem),
        scratch_shapes=[
            pltpu.VMEM((top, rows), jnp.int32),
            pltpu.VMEM((experts, rows), f32),
            pltpu.VMEM((experts, features), bf16),
            pltpu.VMEM((local, features, width), bf16),
            pltpu.VMEM((slots, width), bf16),
            pltpu.VMEM((tokens, features), bf16),
            pltpu.VMEM((groups, experts, half_tokens), bf16),
            pltpu.VMEM((experts, half_tokens), bf16),
            pltpu.VMEM((2, 2, 8, half_tokens), f32),
            pltpu.VMEM((local, tokens, width), bf16),
            pltpu.VMEM((local, tokens, 128), f32),
            pltpu.VMEM((groups, local, rows, width), bf16),
            pltpu.VMEM((groups, local, rows, width), bf16),
            pltpu.VMEM((half_groups, rows, width), f32),
            pltpu.VMEM((local, half_groups, rows, width), bf16),
            pltpu.VMEM((chips, half_groups, rows, width), bf16),
            pltpu.VMEM((groups, local, half_tokens), f32),
            pltpu.VMEM((parts, groups, local, half_tokens), f32),
            pltpu.VMEM((experts, half_tokens), f32),
            dma((5,)), dma((local,)), dma((2 * half_groups,)), dma((groups,)),
            dma((groups - 1,)), dma((groups,)),
            dma((groups,)), dma((groups,)),
            dma((local, half_groups)), dma((chips, half_groups)),
            dma((groups, parts)), dma((parts, groups)),
        ],
        compiler_params=pltpu.CompilerParams(
            collective_id=0, has_side_effects=True, vmem_limit_bytes=40 * 1024 * 1024
        ),
    )(
        expert_ids.T, router_logits.T, out_grad, router_weight, expert_weight,
        hidden_saved.reshape(slots, width),
    )
    weight_grad, hidden, input_grad = pl.pallas_call(
        write_kernel,
        out_shape=out_shape,
        in_specs=[vmem] * 3,
        out_specs=[hbm] * 3,
        scratch_shapes=[dma((2 + 4 * local,))],
    )(*outs)
    return weight_grad, hidden[None], input_grad


def choose(*args):
    out_grad, _, _, _, expert_weight, hidden_saved = args
    groups, parts = lax.axis_size("grp"), lax.axis_size("ep")
    rows, local = out_grad.shape[0], expert_weight.shape[0]
    slots_for_one = hidden_saved.shape[1] // groups
    lanes = groups // 2 * rows
    capacity = slots_for_one // local
    fits = rows <= capacity and lanes % 128 == 0 and lanes <= 256 and local <= 8
    if parts == 2 * local and groups % 2 == 0 and fits and groups & (groups - 1) == 0:
        return fused(*args)
    return body(*args)


def solution(mesh):
    in_specs = (
        P("grp", "ep"),
        P("grp", None),
        P("grp", None),
        P(None, "ep"),
        P("grp", "ep", None),
        P("grp", None, None),
    )
    out_specs = (P("grp", "ep", None), P("grp", "ep", None), P("grp", "ep"))
    return jax.shard_map(choose, mesh=mesh, in_specs=in_specs, out_specs=out_specs, check_vma=False)
```

```python
import jax
import jax.numpy as jnp
from jax import lax
from jax.experimental import pallas as pl
from jax.experimental.pallas import tpu as pltpu
from jax.sharding import PartitionSpec as P

route_scale = 2.5


def body(out_grad, expert_ids, router_logits, router_weight, expert_weight, hidden_saved):
    group_rows, features = out_grad.shape
    top_count = expert_ids.shape[1]
    experts = router_logits.shape[1]
    group_count = lax.axis_size("grp")
    local_experts = expert_weight.shape[0]
    hidden_width = expert_weight.shape[2]
    slot_count = hidden_saved.shape[1]
    capacity = slot_count // (local_experts * group_count)
    expert_span = group_count * capacity
    pair_count = group_rows * top_count
    sig_values = jax.nn.sigmoid(router_logits)
    picked = expert_ids[:, :, None] == jnp.arange(experts, dtype=jnp.int32)[None, None, :]
    chosen = jnp.sum(jnp.where(picked, sig_values[:, None, :], 0.0), axis=2)
    route_probs = route_scale * chosen / jnp.sum(chosen, axis=1, keepdims=True)
    flat_ids = expert_ids.reshape(pair_count)
    onehot = picked.reshape(pair_count, experts).astype(jnp.int32)
    pair_ranks = jnp.sum((jnp.cumsum(onehot, axis=0) - 1) * onehot, axis=1)
    slot_place = (
        flat_ids % local_experts * group_count + flat_ids // local_experts
    ) * capacity + pair_ranks
    slot_match = slot_place[None, :] == jnp.arange(slot_count, dtype=jnp.int32)[:, None]
    token_pick = jnp.sum(
        slot_match.reshape(slot_count, group_rows, top_count).astype(jnp.float32), axis=2
    ).astype(jnp.bfloat16)
    send_rows = jnp.dot(token_pick, out_grad, preferred_element_type=jnp.float32).astype(
        jnp.bfloat16
    )
    send_prob = jnp.sum(
        jnp.where(slot_match, route_probs.reshape(1, pair_count), 0.0), axis=1
    ).astype(jnp.bfloat16)
    got_rows, got_prob = (
        lax.all_to_all(
            send_rows.reshape(local_experts, group_count, capacity, features),
            "grp",
            split_axis=1,
            concat_axis=1,
            tiled=True,
        ),
        lax.all_to_all(
            send_prob.reshape(local_experts, group_count, capacity),
            "grp",
            split_axis=1,
            concat_axis=1,
            tiled=True,
        ),
    )
    slot_grads = got_rows.reshape(local_experts, expert_span, features)
    prob_rows = got_prob.reshape(local_experts, expert_span).astype(jnp.float32)
    saved_rows = hidden_saved.reshape(local_experts, expert_span, hidden_width)
    scaled_rows = (prob_rows[:, :, None] * slot_grads.astype(jnp.float32)).astype(jnp.bfloat16)
    weight_grad = jnp.einsum(
        "lmd,lmf->ldf", scaled_rows, saved_rows, preferred_element_type=jnp.float32
    ).astype(jnp.bfloat16)
    owner_index = lax.axis_index("ep")
    share_rows = slot_count // lax.axis_size("ep")
    flat_prob = prob_rows.reshape(slot_count)
    flat_saved = hidden_saved.reshape(slot_count, hidden_width)
    partial_term = jnp.einsum(
        "lmd,ldf->lmf", slot_grads, expert_weight, preferred_element_type=jnp.float32
    ).reshape(slot_count, hidden_width)
    rounded_term = lax.optimization_barrier(partial_term.astype(jnp.bfloat16)).astype(jnp.float32)
    partial_score = jnp.sum(flat_saved.astype(jnp.float32) * rounded_term, axis=1)
    moved_scores = lax.all_to_all(
        partial_score.reshape(local_experts, group_count, capacity),
        "grp",
        split_axis=1,
        concat_axis=1,
        tiled=True,
    )
    returned = lax.psum(moved_scores, "ep")
    summed = lax.psum_scatter(
        partial_term.astype(jnp.bfloat16), "ep", scatter_dimension=0, tiled=True
    ).astype(jnp.float32)
    own_prob = lax.dynamic_slice_in_dim(flat_prob, owner_index * share_rows, share_rows, 0)
    hidden_grad = (own_prob[:, None] * summed).astype(jnp.bfloat16)[None]
    pair_score = jnp.sum(
        jnp.where(slot_match, returned.reshape(slot_count, 1), 0.0), axis=0
    ).reshape(group_rows, top_count)
    weighted_mean = jnp.sum(route_probs * pair_score, axis=1, keepdims=True) / route_scale
    logit_terms = route_probs * (1.0 - chosen) * (pair_score - weighted_mean)
    router_grad = jnp.sum(jnp.where(picked, logit_terms[:, :, None], 0.0), axis=1).astype(
        jnp.bfloat16
    )
    input_grad = jnp.dot(router_grad, router_weight, preferred_element_type=jnp.float32).astype(
        jnp.bfloat16
    )
    return (weight_grad, hidden_grad, input_grad)


MESH = pl.DeviceIdType.MESH


def flip(a, j):
    out, bit = a, 1
    while bit <= j:
        if j & bit:
            out = out + bit * (1 - 2 * (a // bit % 2))
        bit *= 2
    return out


def fused_kernel(
    ids_hbm, logits_hbm, grad_hbm, rw_hbm, w_hbm, saved_hbm,
    weight_ref, hidden_ref, input_ref,
    ids_ref, logits_ref, rw_ref, w_ref, saved_ref, rows_all, probs_all, probs_own,
    slot_ref, saved_tok, scaled, part, recv_a, total_own, send_b, recv_b,
    score_own, score_recv, score_rows,
    in_sem, w_sem, rows_send, rows_recv, probs_send, probs_recv,
    a_send, a_recv, b_send, b_recv, sc_send, sc_recv,
):
    groups = lax.axis_size("grp")
    parts = lax.axis_size("ep")
    chips = parts // 2
    g = lax.axis_index("grp")
    k = lax.axis_index("ep")
    chip, core = k // 2, k % 2
    experts, rows = logits_ref.shape
    top = ids_ref.shape[0]
    _, local, _, width = part.shape
    features = rows_all.shape[1]
    half_groups = groups // 2
    half_tokens = half_groups * rows
    tokens = groups * rows
    span = saved_ref.shape[0] // local
    share = span // 2
    capacity = span // groups
    f32, bf16 = jnp.float32, jnp.bfloat16
    i32 = jnp.int32
    column, side = g // 2, lax.rem(g, 2)
    mate = g + 1 - 2 * side
    hops = list(range(half_groups - 1, 0, -1))

    barrier = pltpu.get_barrier_semaphore()
    for dg in range(groups):
        for dk in range(parts):
            if dg or dk:
                pl.semaphore_signal(
                    barrier, inc=1,
                    device_id=(lax.rem(g + dg, groups), lax.rem(k + dk, parts)),
                    device_id_type=MESH,
                )

    def block(b):
        return rows_all.at[pl.ds(pl.multiple_of(b * rows, rows), rows), :]

    fetch = [
        pltpu.make_async_copy(src, dst, in_sem.at[i])
        for i, (src, dst) in enumerate([
            (grad_hbm, block(g)), (logits_hbm, logits_ref), (ids_hbm, ids_ref),
            (saved_hbm, saved_ref), (rw_hbm, rw_ref),
        ])
    ]
    w_copies = [
        pltpu.make_async_copy(w_hbm.at[i], w_ref.at[i], w_sem.at[i]) for i in range(local)
    ]
    for copy in [*fetch[:3], *w_copies, *fetch[3:]]:
        copy.start()

    sends = []

    def go(copy, when=None):
        if when is None:
            copy.start()
            sends.append(copy.wait_send)
        else:
            pl.when(when)(copy.start)
            sends.append(lambda: pl.when(when)(copy.wait_send))

    def rows_copy(b, to, sem):
        return pltpu.make_async_remote_copy(
            src_ref=block(b), dst_ref=block(b), send_sem=rows_send.at[sem],
            recv_sem=rows_recv.at[b], device_id=(to, k), device_id_type=MESH,
        )

    def probs_copy(b, to, sem):
        return pltpu.make_async_remote_copy(
            src_ref=probs_own, dst_ref=probs_all.at[b], send_sem=probs_send.at[sem],
            recv_sem=probs_recv.at[b], device_id=(to, k), device_id_type=MESH,
        )

    fetch[0].wait()
    pl.semaphore_wait(barrier, groups * parts - 1)
    go(rows_copy(g, mate, 0))
    for j in hops:
        go(rows_copy(g, flip(column, j) * 2 + side, j))

    fetch[1].wait()
    fetch[2].wait()
    sig = 1.0 / (1.0 + jnp.exp(-logits_ref[...]))
    ids = ids_ref[...]
    expert_iota = lax.broadcasted_iota(i32, (experts, rows), 0)
    named = ids[0:1, :] == expert_iota
    for i in range(1, top):
        named = named | (ids[i : i + 1, :] == expert_iota)
    probs = route_scale * sig / jnp.sum(jnp.where(named, sig, 0.0), axis=0, keepdims=True)
    probs = jnp.where(named, probs, 0.0)
    lane_off = lax.rem(g, half_groups) * rows
    place = (
        lax.broadcasted_iota(i32, (rows, half_tokens), 1)
        == lax.broadcasted_iota(i32, (rows, half_tokens), 0) + lane_off
    )
    placed = jnp.dot(
        probs.astype(bf16), place.astype(f32).astype(bf16), preferred_element_type=f32
    ).astype(bf16)
    probs_own[...] = placed
    probs_all[g] = placed
    for j in range(1, groups):
        go(probs_copy(g, lax.rem(g + j, groups), j - 1))

    order = [lax.rem(chip + 1 + i, chips) for i in range(chips)]
    partner = k + 1 - 2 * core

    def a_copy(b):
        return pltpu.make_async_remote_copy(
            src_ref=part.at[b], dst_ref=recv_a.at[b], send_sem=a_send.at[b],
            recv_sem=a_recv.at[b], device_id=(g, partner), device_id_type=MESH,
        )

    def own(b):
        return b // half_groups == core

    def multiply(b):
        found = block(b)[...]
        for l in range(local):
            part[b, l] = jnp.dot(found, w_ref[l], preferred_element_type=f32).astype(bf16)
        go(a_copy(b), b // half_groups != core)

    def b_copy(b, l, to, source):
        at = lax.rem(b, half_groups)
        return pltpu.make_async_remote_copy(
            src_ref=send_b.at[l, at], dst_ref=recv_b.at[source, at],
            send_sem=b_send.at[l, at], recv_sem=b_recv.at[source, at],
            device_id=(g, to), device_id_type=MESH,
        )

    def finish(b):
        at = lax.rem(b, half_groups)

        @pl.when(own(b))
        def _():
            a_copy(b).wait_recv()
            for l in order[:-1]:
                both = part[b, l].astype(f32) + recv_a[b, l].astype(f32)
                send_b[l, at] = both.astype(bf16)
                b_copy(b, l, l * 2 + core, chip).start()
            total_own[at] = part[b, chip].astype(f32) + recv_a[b, chip].astype(f32)

        def end():
            for l in order[:-1]:
                b_copy(b, l, l * 2 + core, chip).wait_send()

        sends.append(lambda: pl.when(own(b))(end))

    eye = (
        lax.broadcasted_iota(i32, (rows, half_tokens), 0)
        == lax.broadcasted_iota(i32, (rows, half_tokens), 1)
    )

    def score_copy(b, to, y, o):
        return pltpu.make_async_remote_copy(
            src_ref=score_own.at[b], dst_ref=score_recv.at[y, o],
            send_sem=sc_send.at[b, to], recv_sem=sc_recv.at[y, o],
            device_id=(b, to), device_id_type=MESH,
        )

    def score(b, home=False):
        for l in range(local):
            at = pl.ds(pl.multiple_of(b * rows, rows), rows)
            value = jnp.sum(
                saved_tok[l, at, :].astype(f32) * part[b, l].astype(f32), axis=1, keepdims=True
            )
            score_own[b, l : l + 1, :] = jnp.sum(
                jnp.where(eye, value, 0.0), axis=0, keepdims=True
            )
        if home:
            score_recv[k, b] = score_own[b]
        for dk in range(1 if home else 0, parts):
            go(score_copy(b, lax.rem(k + dk, parts), k, g))

    for copy in w_copies:
        copy.wait()
    multiply(g)

    for j in range(1, groups):
        b = lax.rem(g + j, groups)
        probs_copy(b, g, 0).wait_recv()
    pick = (
        lax.broadcasted_iota(i32, (8, experts), 1)
        == lax.broadcasted_iota(i32, (8, experts), 0) + g * local
    ) & (lax.broadcasted_iota(i32, (8, experts), 0) < local)
    pick = pick.astype(f32).astype(bf16)
    lane = lax.broadcasted_iota(i32, (half_tokens, half_tokens), 1)
    line = lax.broadcasted_iota(i32, (half_tokens, half_tokens), 0)
    same = line // rows == lane // rows
    earlier = ((line < lane) & same).astype(f32).astype(bf16)
    later = ((lane < line) & same).astype(f32).astype(bf16)
    unit = (lane == line).astype(f32).astype(bf16)
    lane_block = lax.broadcasted_iota(i32, (8, half_tokens), 1) // rows
    line_block = lax.broadcasted_iota(i32, (half_tokens, 8), 0) // rows
    turn = (((1,), (1,)), ((), ()))
    fetch[3].wait()
    for h in range(2):
        total = probs_all[h * half_groups].astype(f32)
        for b in range(1, half_groups):
            total = total + probs_all[h * half_groups + b].astype(f32)
        mine = jnp.dot(pick, total.astype(bf16), preferred_element_type=f32)
        used = mine > 0.0
        marks = used.astype(f32).astype(bf16)
        rank = jnp.dot(marks, earlier, preferred_element_type=f32)
        slot = lane_block * capacity + rank.astype(i32)
        slot_ref[h, 0] = jnp.where(used, slot, -1).astype(f32)
        slot_ref[h, 1] = mine
        mine_col = lax.dot_general(unit, mine.astype(bf16), turn, preferred_element_type=f32)
        rank_col = lax.dot_general(later, marks, turn, preferred_element_type=f32)
        slot_col = jnp.where(
            mine_col > 0.0, line_block * capacity + rank_col.astype(i32), -1
        )
        spot = lax.broadcasted_iota(i32, (half_tokens, share), 1)
        at = pl.ds(h * half_tokens, half_tokens)
        for l in range(local):
            match = (slot_col[:, l : l + 1] == spot).astype(f32).astype(bf16)
            start = l * span + h * share
            saved_tok[l, at, :] = jnp.dot(
                match, saved_ref[start : start + share, :], preferred_element_type=f32
            ).astype(bf16)
            scaled[l, at, :] = jnp.broadcast_to(
                mine_col[:, l : l + 1], (half_tokens, scaled.shape[2])
            )

    rows_copy(mate, g, 0).wait_recv()
    multiply(mate)
    score(g, home=True)
    finish(g)
    score(mate)
    last = mate
    for j in hops:
        b = flip(column, j) * 2 + side
        rows_copy(b, g, 0).wait_recv()
        go(rows_copy(b, mate, half_groups + j))
        multiply(b)
        finish(last)
        score(b)
        last = b
    for j in hops:
        b = flip(column, j) * 2 + 1 - side
        rows_copy(b, g, 0).wait_recv()
        multiply(b)
        finish(last)
        score(b)
        last = b

    step = min(width, 256)
    for l in range(local):
        weighed = jnp.concatenate(
            [
                (scaled[l, :, 0:128] * rows_all[:, n : n + 128].astype(f32)).astype(bf16)
                for n in range(0, features, 128)
            ],
            axis=1,
        )
        for n in range(0, width, step):
            weight_ref[l, :, n : n + step] = lax.dot_general(
                weighed, saved_tok[l, :, n : n + step], (((0,), (0,)), ((), ())),
                preferred_element_type=f32,
            ).astype(bf16)
        if l == 0:
            finish(last)

    def pick_row(which):
        table = slot_ref[core, which]
        mask = lax.broadcasted_iota(i32, table.shape, 0) == chip
        return jnp.sum(jnp.where(mask, table, 0.0), axis=0, keepdims=True)

    spot = lax.broadcasted_iota(i32, (share, half_tokens), 0).astype(f32)
    spread = jnp.where(spot == pick_row(0), pick_row(1), 0.0).astype(bf16)
    for i in range(chips - 1):
        for at in range(half_groups):
            b_copy(at, 0, k, order[i]).wait_recv()
    total = total_own[...]
    for i in range(chips - 1):
        total = total + recv_b[order[i]].astype(f32)
    hidden_ref[...] = jnp.dot(
        spread, total.reshape(half_tokens, width).astype(bf16), preferred_element_type=f32
    ).astype(bf16)

    for y in range(parts):
        for o in range(groups):
            wait = score_copy(g, k, y, o).wait_recv
            pl.when((o != g) | (y != k))(wait)
    for o in range(groups):
        value = score_recv[0, o]
        for y in range(1, parts):
            value = value + score_recv[y, o]
        score_rows[o * local : (o + 1) * local, :] = value
    pair = score_rows[:, 0:rows]
    mean = jnp.sum(probs * pair, axis=0, keepdims=True) / route_scale
    terms = jnp.where(named, probs * (1.0 - sig) * (pair - mean), 0.0).astype(bf16)
    small = (
        lax.broadcasted_iota(i32, (rows, rows), 0) == lax.broadcasted_iota(i32, (rows, rows), 1)
    )
    turned = lax.dot_general(
        small.astype(f32).astype(bf16), terms, turn, preferred_element_type=f32
    ).astype(bf16)
    fetch[4].wait()
    input_ref[...] = jnp.dot(turned, rw_ref[...], preferred_element_type=f32).astype(bf16)

    for wait in sends:
        wait()


def write_kernel(weight_ref, hidden_ref, input_ref, weight_hbm, hidden_hbm, input_hbm, sem):
    copies = [
        pltpu.make_async_copy(hidden_ref, hidden_hbm, sem.at[0]),
        pltpu.make_async_copy(input_ref, input_hbm, sem.at[1]),
    ]
    local, features, _ = weight_ref.shape
    cut = features // 4
    for l in range(local):
        for n in range(4):
            at = pl.ds(n * cut, cut)
            copies.append(
                pltpu.make_async_copy(
                    weight_ref.at[l, at, :], weight_hbm.at[l, at, :], sem.at[2 + l * 4 + n]
                )
            )
    for copy in copies:
        copy.start()
    for copy in copies:
        copy.wait()


def fused(out_grad, expert_ids, router_logits, router_weight, expert_weight, hidden_saved):
    groups, parts = lax.axis_size("grp"), lax.axis_size("ep")
    rows, features = out_grad.shape
    experts = router_logits.shape[1]
    top = expert_ids.shape[1]
    local, _, width = expert_weight.shape
    slots = hidden_saved.shape[1]
    span = slots // local
    half_groups = groups // 2
    half_tokens = half_groups * rows
    tokens = groups * rows
    share = span // 2
    chips = parts // 2
    f32, bf16 = jnp.float32, jnp.bfloat16
    vmem = pl.BlockSpec(memory_space=pltpu.VMEM)
    hbm = pl.BlockSpec(memory_space=pltpu.HBM)
    dma = pltpu.SemaphoreType.DMA
    out_shape = (
        jax.ShapeDtypeStruct((local, features, width), bf16),
        jax.ShapeDtypeStruct((share, width), bf16),
        jax.ShapeDtypeStruct((rows, features), bf16),
    )
    pin = pltpu.with_memory_space_constraint
    outs = pl.pallas_call(
        fused_kernel,
        out_shape=tuple(pltpu.VMEM(x.shape, x.dtype) for x in out_shape),
        in_specs=[hbm] * 6,
        out_specs=(vmem, vmem, vmem),
        scratch_shapes=[
            pltpu.VMEM((top, rows), jnp.int32),
            pltpu.VMEM((experts, rows), f32),
            pltpu.VMEM((experts, features), bf16),
            pltpu.VMEM((local, features, width), bf16),
            pltpu.VMEM((slots, width), bf16),
            pltpu.VMEM((tokens, features), bf16),
            pltpu.VMEM((groups, experts, half_tokens), bf16),
            pltpu.VMEM((experts, half_tokens), bf16),
            pltpu.VMEM((2, 2, 8, half_tokens), f32),
            pltpu.VMEM((local, tokens, width), bf16),
            pltpu.VMEM((local, tokens, 128), f32),
            pltpu.VMEM((groups, local, rows, width), bf16),
            pltpu.VMEM((groups, local, rows, width), bf16),
            pltpu.VMEM((half_groups, rows, width), f32),
            pltpu.VMEM((local, half_groups, rows, width), bf16),
            pltpu.VMEM((chips, half_groups, rows, width), bf16),
            pltpu.VMEM((groups, local, half_tokens), f32),
            pltpu.VMEM((parts, groups, local, half_tokens), f32),
            pltpu.VMEM((experts, half_tokens), f32),
            dma((5,)), dma((local,)), dma((2 * half_groups,)), dma((groups,)),
            dma((groups - 1,)), dma((groups,)),
            dma((groups,)), dma((groups,)),
            dma((local, half_groups)), dma((chips, half_groups)),
            dma((groups, parts)), dma((parts, groups)),
        ],
        compiler_params=pltpu.CompilerParams(
            collective_id=0, has_side_effects=True, vmem_limit_bytes=40 * 1024 * 1024
        ),
    )(*[
        pin(x, pltpu.HBM)
        for x in (
            expert_ids.T, router_logits.T, out_grad, router_weight, expert_weight,
            hidden_saved.reshape(slots, width),
        )
    ])
    weight_grad, hidden, input_grad = pl.pallas_call(
        write_kernel,
        out_shape=out_shape,
        in_specs=[vmem] * 3,
        out_specs=[hbm] * 3,
        scratch_shapes=[dma((2 + 4 * local,))],
        compiler_params=pltpu.CompilerParams(vmem_limit_bytes=16 * 1024 * 1024),
    )(*[pin(x, pltpu.VMEM) for x in outs])
    return weight_grad, hidden[None], input_grad


def choose(*args):
    out_grad, _, _, _, expert_weight, hidden_saved = args
    groups, parts = lax.axis_size("grp"), lax.axis_size("ep")
    rows, local = out_grad.shape[0], expert_weight.shape[0]
    slots_for_one = hidden_saved.shape[1] // groups
    lanes = groups // 2 * rows
    capacity = slots_for_one // local
    fits = rows <= capacity and lanes % 128 == 0 and lanes <= 256 and local <= 8
    if parts == 2 * local and groups % 2 == 0 and fits and groups & (groups - 1) == 0:
        return fused(*args)
    return body(*args)


def solution(mesh):
    in_specs = (
        P("grp", "ep"),
        P("grp", None),
        P("grp", None),
        P(None, "ep"),
        P("grp", "ep", None),
        P("grp", None, None),
    )
    out_specs = (P("grp", "ep", None), P("grp", "ep", None), P("grp", "ep"))
    return jax.shard_map(choose, mesh=mesh, in_specs=in_specs, out_specs=out_specs, check_vma=False)
```

```python
import jax
import jax.numpy as jnp
from jax import lax
from jax.experimental import pallas as pl
from jax.experimental.pallas import tpu as pltpu
from jax.sharding import PartitionSpec as P

route_scale = 2.5


def body(out_grad, expert_ids, router_logits, router_weight, expert_weight, hidden_saved):
    group_rows, features = out_grad.shape
    top_count = expert_ids.shape[1]
    experts = router_logits.shape[1]
    group_count = lax.axis_size("grp")
    local_experts = expert_weight.shape[0]
    hidden_width = expert_weight.shape[2]
    slot_count = hidden_saved.shape[1]
    capacity = slot_count // (local_experts * group_count)
    expert_span = group_count * capacity
    pair_count = group_rows * top_count
    sig_values = jax.nn.sigmoid(router_logits)
    picked = expert_ids[:, :, None] == jnp.arange(experts, dtype=jnp.int32)[None, None, :]
    chosen = jnp.sum(jnp.where(picked, sig_values[:, None, :], 0.0), axis=2)
    route_probs = route_scale * chosen / jnp.sum(chosen, axis=1, keepdims=True)
    flat_ids = expert_ids.reshape(pair_count)
    onehot = picked.reshape(pair_count, experts).astype(jnp.int32)
    pair_ranks = jnp.sum((jnp.cumsum(onehot, axis=0) - 1) * onehot, axis=1)
    slot_place = (
        flat_ids % local_experts * group_count + flat_ids // local_experts
    ) * capacity + pair_ranks
    slot_match = slot_place[None, :] == jnp.arange(slot_count, dtype=jnp.int32)[:, None]
    token_pick = jnp.sum(
        slot_match.reshape(slot_count, group_rows, top_count).astype(jnp.float32), axis=2
    ).astype(jnp.bfloat16)
    send_rows = jnp.dot(token_pick, out_grad, preferred_element_type=jnp.float32).astype(
        jnp.bfloat16
    )
    send_prob = jnp.sum(
        jnp.where(slot_match, route_probs.reshape(1, pair_count), 0.0), axis=1
    ).astype(jnp.bfloat16)
    got_rows, got_prob = (
        lax.all_to_all(
            send_rows.reshape(local_experts, group_count, capacity, features),
            "grp",
            split_axis=1,
            concat_axis=1,
            tiled=True,
        ),
        lax.all_to_all(
            send_prob.reshape(local_experts, group_count, capacity),
            "grp",
            split_axis=1,
            concat_axis=1,
            tiled=True,
        ),
    )
    slot_grads = got_rows.reshape(local_experts, expert_span, features)
    prob_rows = got_prob.reshape(local_experts, expert_span).astype(jnp.float32)
    saved_rows = hidden_saved.reshape(local_experts, expert_span, hidden_width)
    scaled_rows = (prob_rows[:, :, None] * slot_grads.astype(jnp.float32)).astype(jnp.bfloat16)
    weight_grad = jnp.einsum(
        "lmd,lmf->ldf", scaled_rows, saved_rows, preferred_element_type=jnp.float32
    ).astype(jnp.bfloat16)
    owner_index = lax.axis_index("ep")
    share_rows = slot_count // lax.axis_size("ep")
    flat_prob = prob_rows.reshape(slot_count)
    flat_saved = hidden_saved.reshape(slot_count, hidden_width)
    partial_term = jnp.einsum(
        "lmd,ldf->lmf", slot_grads, expert_weight, preferred_element_type=jnp.float32
    ).reshape(slot_count, hidden_width)
    rounded_term = lax.optimization_barrier(partial_term.astype(jnp.bfloat16)).astype(jnp.float32)
    partial_score = jnp.sum(flat_saved.astype(jnp.float32) * rounded_term, axis=1)
    moved_scores = lax.all_to_all(
        partial_score.reshape(local_experts, group_count, capacity),
        "grp",
        split_axis=1,
        concat_axis=1,
        tiled=True,
    )
    returned = lax.psum(moved_scores, "ep")
    summed = lax.psum_scatter(
        partial_term.astype(jnp.bfloat16), "ep", scatter_dimension=0, tiled=True
    ).astype(jnp.float32)
    own_prob = lax.dynamic_slice_in_dim(flat_prob, owner_index * share_rows, share_rows, 0)
    hidden_grad = (own_prob[:, None] * summed).astype(jnp.bfloat16)[None]
    pair_score = jnp.sum(
        jnp.where(slot_match, returned.reshape(slot_count, 1), 0.0), axis=0
    ).reshape(group_rows, top_count)
    weighted_mean = jnp.sum(route_probs * pair_score, axis=1, keepdims=True) / route_scale
    logit_terms = route_probs * (1.0 - chosen) * (pair_score - weighted_mean)
    router_grad = jnp.sum(jnp.where(picked, logit_terms[:, :, None], 0.0), axis=1).astype(
        jnp.bfloat16
    )
    input_grad = jnp.dot(router_grad, router_weight, preferred_element_type=jnp.float32).astype(
        jnp.bfloat16
    )
    return (weight_grad, hidden_grad, input_grad)


MESH = pl.DeviceIdType.MESH


def flip(a, j):
    out, bit = a, 1
    while bit <= j:
        if j & bit:
            out = out + bit * (1 - 2 * (a // bit % 2))
        bit *= 2
    return out


def fused_kernel(
    ids_hbm, logits_hbm, grad_hbm, rw_hbm, w_hbm, saved_hbm,
    weight_ref, hidden_ref, input_ref,
    ids_ref, logits_ref, rw_ref, w_ref, saved_ref, rows_all, probs_all, probs_own,
    slot_ref, saved_tok, scaled, part, recv_a, total_own, send_b, recv_b,
    score_own, score_recv, score_rows,
    in_sem, w_sem, rows_send, rows_recv, probs_send, probs_recv,
    a_send, a_recv, b_send, b_recv, sc_send, sc_recv,
):
    groups = lax.axis_size("grp")
    parts = lax.axis_size("ep")
    chips = parts // 2
    g = lax.axis_index("grp")
    k = lax.axis_index("ep")
    chip, core = k // 2, k % 2
    experts, rows = logits_ref.shape
    top = ids_ref.shape[0]
    _, local, _, width = part.shape
    features = rows_all.shape[1]
    half_groups = groups // 2
    half_tokens = half_groups * rows
    tokens = groups * rows
    span = saved_ref.shape[0] // local
    share = span // 2
    capacity = span // groups
    f32, bf16 = jnp.float32, jnp.bfloat16
    i32 = jnp.int32
    column, side = g // 2, lax.rem(g, 2)
    mate = g + 1 - 2 * side
    hops = list(range(half_groups - 1, 0, -1))

    barrier = pltpu.get_barrier_semaphore()
    peers = [(lax.rem(g + j, groups), k) for j in range(1, groups)]
    peers += [(g, lax.rem(k + j, parts)) for j in range(1, parts)]
    for peer in peers:
        pl.semaphore_signal(barrier, inc=1, device_id=peer, device_id_type=MESH)

    def block(b):
        return rows_all.at[pl.ds(pl.multiple_of(b * rows, rows), rows), :]

    fetch = [
        pltpu.make_async_copy(src, dst, in_sem.at[i])
        for i, (src, dst) in enumerate([
            (grad_hbm, block(g)), (logits_hbm, logits_ref), (ids_hbm, ids_ref),
            (saved_hbm, saved_ref), (rw_hbm, rw_ref),
        ])
    ]
    w_copies = [
        pltpu.make_async_copy(w_hbm.at[i], w_ref.at[i], w_sem.at[i]) for i in range(local)
    ]
    for copy in [*fetch[1:3], fetch[0], *w_copies, *fetch[3:]]:
        copy.start()

    sends = []

    def go(copy, when=None):
        if when is None:
            copy.start()
            sends.append(copy.wait_send)
        else:
            pl.when(when)(copy.start)
            sends.append(lambda: pl.when(when)(copy.wait_send))

    def rows_copy(b, to, sem):
        return pltpu.make_async_remote_copy(
            src_ref=block(b), dst_ref=block(b), send_sem=rows_send.at[sem],
            recv_sem=rows_recv.at[b], device_id=(to, k), device_id_type=MESH,
        )

    def probs_copy(b, to, sem):
        return pltpu.make_async_remote_copy(
            src_ref=probs_own, dst_ref=probs_all.at[b], send_sem=probs_send.at[sem],
            recv_sem=probs_recv.at[b], device_id=(to, k), device_id_type=MESH,
        )

    fetch[1].wait()
    fetch[2].wait()
    sig = 1.0 / (1.0 + jnp.exp(-logits_ref[...]))
    ids = ids_ref[...]
    expert_iota = lax.broadcasted_iota(i32, (experts, rows), 0)
    named = ids[0:1, :] == expert_iota
    for i in range(1, top):
        named = named | (ids[i : i + 1, :] == expert_iota)
    probs = route_scale * sig / jnp.sum(jnp.where(named, sig, 0.0), axis=0, keepdims=True)
    probs = jnp.where(named, probs, 0.0)
    lane_off = lax.rem(g, half_groups) * rows
    place = (
        lax.broadcasted_iota(i32, (rows, half_tokens), 1)
        == lax.broadcasted_iota(i32, (rows, half_tokens), 0) + lane_off
    )
    placed = jnp.dot(
        probs.astype(bf16), place.astype(f32).astype(bf16), preferred_element_type=f32
    ).astype(bf16)
    probs_own[...] = placed
    probs_all[g] = placed
    fetch[0].wait()
    pl.semaphore_wait(barrier, len(peers))
    for j in range(1, groups):
        go(probs_copy(g, lax.rem(g + j, groups), j - 1))
    go(rows_copy(g, mate, 0))
    for j in hops:
        go(rows_copy(g, flip(column, j) * 2 + side, j))

    order = [lax.rem(chip + 1 + i, chips) for i in range(chips)]
    partner = k + 1 - 2 * core

    def a_copy(b):
        return pltpu.make_async_remote_copy(
            src_ref=part.at[b], dst_ref=recv_a.at[b], send_sem=a_send.at[b],
            recv_sem=a_recv.at[b], device_id=(g, partner), device_id_type=MESH,
        )

    def own(b):
        return b // half_groups == core

    def multiply(b):
        found = block(b)[...]
        for l in range(local):
            part[b, l] = jnp.dot(found, w_ref[l], preferred_element_type=f32).astype(bf16)
        go(a_copy(b), b // half_groups != core)

    def b_copy(b, l, to, source):
        at = lax.rem(b, half_groups)
        return pltpu.make_async_remote_copy(
            src_ref=send_b.at[l, at], dst_ref=recv_b.at[source, at],
            send_sem=b_send.at[l, at], recv_sem=b_recv.at[source, at],
            device_id=(g, to), device_id_type=MESH,
        )

    def finish(b):
        at = lax.rem(b, half_groups)

        @pl.when(own(b))
        def _():
            a_copy(b).wait_recv()
            for l in order[:-1]:
                both = part[b, l].astype(f32) + recv_a[b, l].astype(f32)
                send_b[l, at] = both.astype(bf16)
                b_copy(b, l, l * 2 + core, chip).start()
            total_own[at] = part[b, chip].astype(f32) + recv_a[b, chip].astype(f32)

        def end():
            for l in order[:-1]:
                b_copy(b, l, l * 2 + core, chip).wait_send()

        sends.append(lambda: pl.when(own(b))(end))

    eye = (
        lax.broadcasted_iota(i32, (rows, half_tokens), 0)
        == lax.broadcasted_iota(i32, (rows, half_tokens), 1)
    )

    def score_copy(b, to, y, o):
        return pltpu.make_async_remote_copy(
            src_ref=score_own.at[b], dst_ref=score_recv.at[y, o],
            send_sem=sc_send.at[b, to], recv_sem=sc_recv.at[y, o],
            device_id=(b, to), device_id_type=MESH,
        )

    def score(b, home=False):
        for l in range(local):
            at = pl.ds(pl.multiple_of(b * rows, rows), rows)
            value = jnp.sum(
                saved_tok[l, at, :].astype(f32) * part[b, l].astype(f32), axis=1, keepdims=True
            )
            score_own[b, l : l + 1, :] = jnp.sum(
                jnp.where(eye, value, 0.0), axis=0, keepdims=True
            )
        if home:
            score_recv[k, b] = score_own[b]
        for dk in range(1 if home else 0, parts):
            go(score_copy(b, lax.rem(k + dk, parts), k, g))

    for copy in w_copies:
        copy.wait()
    multiply(g)

    for j in range(1, groups):
        b = lax.rem(g + j, groups)
        probs_copy(b, g, 0).wait_recv()
    pick = (
        lax.broadcasted_iota(i32, (8, experts), 1)
        == lax.broadcasted_iota(i32, (8, experts), 0) + g * local
    ) & (lax.broadcasted_iota(i32, (8, experts), 0) < local)
    pick = pick.astype(f32).astype(bf16)
    lane = lax.broadcasted_iota(i32, (half_tokens, half_tokens), 1)
    line = lax.broadcasted_iota(i32, (half_tokens, half_tokens), 0)
    same = line // rows == lane // rows
    earlier = ((line < lane) & same).astype(f32).astype(bf16)
    later = ((lane < line) & same).astype(f32).astype(bf16)
    unit = (lane == line).astype(f32).astype(bf16)
    lane_block = lax.broadcasted_iota(i32, (8, half_tokens), 1) // rows
    line_block = lax.broadcasted_iota(i32, (half_tokens, 8), 0) // rows
    turn = (((1,), (1,)), ((), ()))
    fetch[3].wait()
    for h in range(2):
        total = probs_all[h * half_groups].astype(f32)
        for b in range(1, half_groups):
            total = total + probs_all[h * half_groups + b].astype(f32)
        mine = jnp.dot(pick, total.astype(bf16), preferred_element_type=f32)
        used = mine > 0.0
        marks = used.astype(f32).astype(bf16)
        rank = jnp.dot(marks, earlier, preferred_element_type=f32)
        slot = lane_block * capacity + rank.astype(i32)
        slot_ref[h, 0] = jnp.where(used, slot, -1).astype(f32)
        slot_ref[h, 1] = mine
        mine_col = lax.dot_general(unit, mine.astype(bf16), turn, preferred_element_type=f32)
        rank_col = lax.dot_general(later, marks, turn, preferred_element_type=f32)
        slot_col = jnp.where(
            mine_col > 0.0, line_block * capacity + rank_col.astype(i32), -1
        )
        spot = lax.broadcasted_iota(i32, (half_tokens, share), 1)
        at = pl.ds(h * half_tokens, half_tokens)
        for l in range(local):
            match = (slot_col[:, l : l + 1] == spot).astype(f32).astype(bf16)
            start = l * span + h * share
            saved_tok[l, at, :] = jnp.dot(
                match, saved_ref[start : start + share, :], preferred_element_type=f32
            ).astype(bf16)
            scaled[l, at, :] = jnp.broadcast_to(
                mine_col[:, l : l + 1], (half_tokens, scaled.shape[2])
            )

    rows_copy(mate, g, 0).wait_recv()
    multiply(mate)
    score(g, home=True)
    finish(g)
    score(mate)
    last = mate
    for j in hops:
        b = flip(column, j) * 2 + side
        rows_copy(b, g, 0).wait_recv()
        go(rows_copy(b, mate, half_groups + j))
        multiply(b)
        finish(last)
        score(b)
        last = b
    for j in hops:
        b = flip(column, j) * 2 + 1 - side
        rows_copy(b, g, 0).wait_recv()
        multiply(b)
        finish(last)
        score(b)
        last = b

    step = min(width, 256)
    for l in range(local):
        weighed = jnp.concatenate(
            [
                (scaled[l, :, 0:128] * rows_all[:, n : n + 128].astype(f32)).astype(bf16)
                for n in range(0, features, 128)
            ],
            axis=1,
        )
        for n in range(0, width, step):
            weight_ref[l, :, n : n + step] = lax.dot_general(
                weighed, saved_tok[l, :, n : n + step], (((0,), (0,)), ((), ())),
                preferred_element_type=f32,
            ).astype(bf16)
        if l == 0:
            finish(last)

    def pick_row(which):
        table = slot_ref[core, which]
        mask = lax.broadcasted_iota(i32, table.shape, 0) == chip
        return jnp.sum(jnp.where(mask, table, 0.0), axis=0, keepdims=True)

    spot = lax.broadcasted_iota(i32, (share, half_tokens), 0).astype(f32)
    spread = jnp.where(spot == pick_row(0), pick_row(1), 0.0).astype(bf16)
    for i in range(chips - 1):
        for at in range(half_groups):
            b_copy(at, 0, k, order[i]).wait_recv()
    total = total_own[...]
    for i in range(chips - 1):
        total = total + recv_b[order[i]].astype(f32)
    hidden_ref[...] = jnp.dot(
        spread, total.reshape(half_tokens, width).astype(bf16), preferred_element_type=f32
    ).astype(bf16)

    for y in range(parts):
        for o in range(groups):
            wait = score_copy(g, k, y, o).wait_recv
            pl.when((o != g) | (y != k))(wait)
    for o in range(groups):
        value = score_recv[0, o]
        for y in range(1, parts):
            value = value + score_recv[y, o]
        score_rows[o * local : (o + 1) * local, :] = value
    pair = score_rows[:, 0:rows]
    mean = jnp.sum(probs * pair, axis=0, keepdims=True) / route_scale
    terms = jnp.where(named, probs * (1.0 - sig) * (pair - mean), 0.0).astype(bf16)
    small = (
        lax.broadcasted_iota(i32, (rows, rows), 0) == lax.broadcasted_iota(i32, (rows, rows), 1)
    )
    turned = lax.dot_general(
        small.astype(f32).astype(bf16), terms, turn, preferred_element_type=f32
    ).astype(bf16)
    fetch[4].wait()
    input_ref[...] = jnp.dot(turned, rw_ref[...], preferred_element_type=f32).astype(bf16)

    for wait in sends:
        wait()


def write_kernel(weight_ref, hidden_ref, input_ref, weight_hbm, hidden_hbm, input_hbm, sem):
    copies = [
        pltpu.make_async_copy(hidden_ref, hidden_hbm, sem.at[0]),
        pltpu.make_async_copy(input_ref, input_hbm, sem.at[1]),
    ]
    local, features, _ = weight_ref.shape
    cut = features // 4
    for l in range(local):
        for n in range(4):
            at = pl.ds(n * cut, cut)
            copies.append(
                pltpu.make_async_copy(
                    weight_ref.at[l, at, :], weight_hbm.at[l, at, :], sem.at[2 + l * 4 + n]
                )
            )
    for copy in copies:
        copy.start()
    for copy in copies:
        copy.wait()


def fused(out_grad, expert_ids, router_logits, router_weight, expert_weight, hidden_saved):
    groups, parts = lax.axis_size("grp"), lax.axis_size("ep")
    rows, features = out_grad.shape
    experts = router_logits.shape[1]
    top = expert_ids.shape[1]
    local, _, width = expert_weight.shape
    slots = hidden_saved.shape[1]
    span = slots // local
    half_groups = groups // 2
    half_tokens = half_groups * rows
    tokens = groups * rows
    share = span // 2
    chips = parts // 2
    f32, bf16 = jnp.float32, jnp.bfloat16
    vmem = pl.BlockSpec(memory_space=pltpu.VMEM)
    hbm = pl.BlockSpec(memory_space=pltpu.HBM)
    dma = pltpu.SemaphoreType.DMA
    out_shape = (
        jax.ShapeDtypeStruct((local, features, width), bf16),
        jax.ShapeDtypeStruct((share, width), bf16),
        jax.ShapeDtypeStruct((rows, features), bf16),
    )
    pin = pltpu.with_memory_space_constraint
    outs = pl.pallas_call(
        fused_kernel,
        out_shape=tuple(pltpu.VMEM(x.shape, x.dtype) for x in out_shape),
        in_specs=[hbm] * 6,
        out_specs=(vmem, vmem, vmem),
        scratch_shapes=[
            pltpu.VMEM((top, rows), jnp.int32),
            pltpu.VMEM((experts, rows), f32),
            pltpu.VMEM((experts, features), bf16),
            pltpu.VMEM((local, features, width), bf16),
            pltpu.VMEM((slots, width), bf16),
            pltpu.VMEM((tokens, features), bf16),
            pltpu.VMEM((groups, experts, half_tokens), bf16),
            pltpu.VMEM((experts, half_tokens), bf16),
            pltpu.VMEM((2, 2, 8, half_tokens), f32),
            pltpu.VMEM((local, tokens, width), bf16),
            pltpu.VMEM((local, tokens, 128), f32),
            pltpu.VMEM((groups, local, rows, width), bf16),
            pltpu.VMEM((groups, local, rows, width), bf16),
            pltpu.VMEM((half_groups, rows, width), f32),
            pltpu.VMEM((local, half_groups, rows, width), bf16),
            pltpu.VMEM((chips, half_groups, rows, width), bf16),
            pltpu.VMEM((groups, local, half_tokens), f32),
            pltpu.VMEM((parts, groups, local, half_tokens), f32),
            pltpu.VMEM((experts, half_tokens), f32),
            dma((5,)), dma((local,)), dma((2 * half_groups,)), dma((groups,)),
            dma((groups - 1,)), dma((groups,)),
            dma((groups,)), dma((groups,)),
            dma((local, half_groups)), dma((chips, half_groups)),
            dma((groups, parts)), dma((parts, groups)),
        ],
        compiler_params=pltpu.CompilerParams(
            collective_id=0, has_side_effects=True, vmem_limit_bytes=40 * 1024 * 1024
        ),
    )(*[
        pin(x, pltpu.HBM)
        for x in (
            expert_ids.T, router_logits.T, out_grad, router_weight, expert_weight,
            hidden_saved.reshape(slots, width),
        )
    ])
    weight_grad, hidden, input_grad = pl.pallas_call(
        write_kernel,
        out_shape=out_shape,
        in_specs=[vmem] * 3,
        out_specs=[hbm] * 3,
        scratch_shapes=[dma((2 + 4 * local,))],
        compiler_params=pltpu.CompilerParams(vmem_limit_bytes=16 * 1024 * 1024),
    )(*[pin(x, pltpu.VMEM) for x in outs])
    return weight_grad, hidden[None], input_grad


def choose(*args):
    out_grad, _, _, _, expert_weight, hidden_saved = args
    groups, parts = lax.axis_size("grp"), lax.axis_size("ep")
    rows, local = out_grad.shape[0], expert_weight.shape[0]
    slots_for_one = hidden_saved.shape[1] // groups
    lanes = groups // 2 * rows
    capacity = slots_for_one // local
    fits = rows <= capacity and lanes % 128 == 0 and lanes <= 256 and local <= 8
    if parts == 2 * local and groups % 2 == 0 and fits and groups & (groups - 1) == 0:
        return fused(*args)
    return body(*args)


def solution(mesh):
    in_specs = (
        P("grp", "ep"),
        P("grp", None),
        P("grp", None),
        P(None, "ep"),
        P("grp", "ep", None),
        P("grp", None, None),
    )
    out_specs = (P("grp", "ep", None), P("grp", "ep", None), P("grp", "ep"))
    return jax.shard_map(choose, mesh=mesh, in_specs=in_specs, out_specs=out_specs, check_vma=False)
```

```python
import jax
import jax.numpy as jnp
from jax import lax
from jax.experimental import pallas as pl
from jax.experimental.pallas import tpu as pltpu
from jax.sharding import PartitionSpec as P

route_scale = 2.5


def body(out_grad, expert_ids, router_logits, router_weight, expert_weight, hidden_saved):
    group_rows, features = out_grad.shape
    top_count = expert_ids.shape[1]
    experts = router_logits.shape[1]
    group_count = lax.axis_size("grp")
    local_experts = expert_weight.shape[0]
    hidden_width = expert_weight.shape[2]
    slot_count = hidden_saved.shape[1]
    capacity = slot_count // (local_experts * group_count)
    expert_span = group_count * capacity
    pair_count = group_rows * top_count
    sig_values = jax.nn.sigmoid(router_logits)
    picked = expert_ids[:, :, None] == jnp.arange(experts, dtype=jnp.int32)[None, None, :]
    chosen = jnp.sum(jnp.where(picked, sig_values[:, None, :], 0.0), axis=2)
    route_probs = route_scale * chosen / jnp.sum(chosen, axis=1, keepdims=True)
    flat_ids = expert_ids.reshape(pair_count)
    onehot = picked.reshape(pair_count, experts).astype(jnp.int32)
    pair_ranks = jnp.sum((jnp.cumsum(onehot, axis=0) - 1) * onehot, axis=1)
    slot_place = (
        flat_ids % local_experts * group_count + flat_ids // local_experts
    ) * capacity + pair_ranks
    slot_match = slot_place[None, :] == jnp.arange(slot_count, dtype=jnp.int32)[:, None]
    token_pick = jnp.sum(
        slot_match.reshape(slot_count, group_rows, top_count).astype(jnp.float32), axis=2
    ).astype(jnp.bfloat16)
    send_rows = jnp.dot(token_pick, out_grad, preferred_element_type=jnp.float32).astype(
        jnp.bfloat16
    )
    send_prob = jnp.sum(
        jnp.where(slot_match, route_probs.reshape(1, pair_count), 0.0), axis=1
    ).astype(jnp.bfloat16)
    got_rows, got_prob = (
        lax.all_to_all(
            send_rows.reshape(local_experts, group_count, capacity, features),
            "grp",
            split_axis=1,
            concat_axis=1,
            tiled=True,
        ),
        lax.all_to_all(
            send_prob.reshape(local_experts, group_count, capacity),
            "grp",
            split_axis=1,
            concat_axis=1,
            tiled=True,
        ),
    )
    slot_grads = got_rows.reshape(local_experts, expert_span, features)
    prob_rows = got_prob.reshape(local_experts, expert_span).astype(jnp.float32)
    saved_rows = hidden_saved.reshape(local_experts, expert_span, hidden_width)
    scaled_rows = (prob_rows[:, :, None] * slot_grads.astype(jnp.float32)).astype(jnp.bfloat16)
    weight_grad = jnp.einsum(
        "lmd,lmf->ldf", scaled_rows, saved_rows, preferred_element_type=jnp.float32
    ).astype(jnp.bfloat16)
    owner_index = lax.axis_index("ep")
    share_rows = slot_count // lax.axis_size("ep")
    flat_prob = prob_rows.reshape(slot_count)
    flat_saved = hidden_saved.reshape(slot_count, hidden_width)
    partial_term = jnp.einsum(
        "lmd,ldf->lmf", slot_grads, expert_weight, preferred_element_type=jnp.float32
    ).reshape(slot_count, hidden_width)
    rounded_term = lax.optimization_barrier(partial_term.astype(jnp.bfloat16)).astype(jnp.float32)
    partial_score = jnp.sum(flat_saved.astype(jnp.float32) * rounded_term, axis=1)
    moved_scores = lax.all_to_all(
        partial_score.reshape(local_experts, group_count, capacity),
        "grp",
        split_axis=1,
        concat_axis=1,
        tiled=True,
    )
    returned = lax.psum(moved_scores, "ep")
    summed = lax.psum_scatter(
        partial_term.astype(jnp.bfloat16), "ep", scatter_dimension=0, tiled=True
    ).astype(jnp.float32)
    own_prob = lax.dynamic_slice_in_dim(flat_prob, owner_index * share_rows, share_rows, 0)
    hidden_grad = (own_prob[:, None] * summed).astype(jnp.bfloat16)[None]
    pair_score = jnp.sum(
        jnp.where(slot_match, returned.reshape(slot_count, 1), 0.0), axis=0
    ).reshape(group_rows, top_count)
    weighted_mean = jnp.sum(route_probs * pair_score, axis=1, keepdims=True) / route_scale
    logit_terms = route_probs * (1.0 - chosen) * (pair_score - weighted_mean)
    router_grad = jnp.sum(jnp.where(picked, logit_terms[:, :, None], 0.0), axis=1).astype(
        jnp.bfloat16
    )
    input_grad = jnp.dot(router_grad, router_weight, preferred_element_type=jnp.float32).astype(
        jnp.bfloat16
    )
    return (weight_grad, hidden_grad, input_grad)


MESH = pl.DeviceIdType.MESH


def flip(a, j):
    out, bit = a, 1
    while bit <= j:
        if j & bit:
            out = out + bit * (1 - 2 * (a // bit % 2))
        bit *= 2
    return out


def fused_kernel(
    ids_hbm, logits_hbm, grad_hbm, rw_hbm, w_hbm, saved_hbm,
    weight_ref, hidden_ref, input_ref,
    ids_ref, logits_ref, rw_ref, w_ref, saved_ref, rows_all, notes_own, notes_all,
    spread_ref, saved_tok, scaled, part, recv_a, send_b, recv_b,
    score_own, score_recv, score_rows,
    in_sem, w_sem, rows_send, rows_recv, note_send, note_recv,
    a_send, a_recv, kept_recv, b_send, b_recv, sc_send, sc_recv,
):
    groups = lax.axis_size("grp")
    parts = lax.axis_size("ep")
    chips = parts // 2
    g = lax.axis_index("grp")
    k = lax.axis_index("ep")
    chip, core = k // 2, k % 2
    experts, rows = logits_ref.shape
    top = ids_ref.shape[0]
    _, local, _, width = part.shape
    features = rows_all.shape[1]
    half_groups = groups // 2
    half_tokens = half_groups * rows
    tokens = groups * rows
    span = saved_ref.shape[0] // local
    share = span // 2
    capacity = span // groups
    f32, bf16 = jnp.float32, jnp.bfloat16
    column, side = g // 2, lax.rem(g, 2)
    mate = g + 1 - 2 * side
    hops = list(range(half_groups - 1, 0, -1))
    turn = (((1,), (1,)), ((), ()))

    def iota(shape, dim):
        return lax.broadcasted_iota(jnp.int32, shape, dim)

    def mark(mask):
        return mask.astype(f32).astype(bf16)

    def dot(a, b):
        return jnp.dot(a, b, preferred_element_type=f32)

    barrier = pltpu.get_barrier_semaphore()
    peers = [(lax.rem(g + j, groups), k) for j in range(1, groups)]
    peers += [(g, lax.rem(k + j, parts)) for j in range(1, parts)]
    for peer in peers:
        pl.semaphore_signal(barrier, inc=1, device_id=peer, device_id_type=MESH)

    def block(b):
        return rows_all.at[pl.ds(pl.multiple_of(b * rows, rows), rows), :]

    fetch = [
        pltpu.make_async_copy(src, dst, in_sem.at[i])
        for i, (src, dst) in enumerate([
            (grad_hbm, block(g)), (logits_hbm, logits_ref), (ids_hbm, ids_ref),
            (saved_hbm, saved_ref), (rw_hbm, rw_ref),
        ])
    ]
    w_copy = pltpu.make_async_copy(w_hbm, w_ref, w_sem)
    for copy in [*fetch[1:3], fetch[0], w_copy, *fetch[3:]]:
        copy.start()

    def remote(src, dst, send, recv, to):
        return pltpu.make_async_remote_copy(
            src_ref=src, dst_ref=dst, send_sem=send, recv_sem=recv, device_id=to,
            device_id_type=MESH,
        )

    def rows_copy(b, to):
        return remote(block(b), block(b), rows_send, rows_recv.at[b], (to, k))

    def note_copy(b, to):
        return remote(notes_own.at[to], notes_all.at[b], note_send, note_recv, (to, k))

    fetch[1].wait()
    fetch[2].wait()
    sig = 1.0 / (1.0 + jnp.exp(-logits_ref[...]))
    ids = ids_ref[...]
    expert_iota = iota((experts, rows), 0)
    named = ids[0:1, :] == expert_iota
    for i in range(1, top):
        named = named | (ids[i : i + 1, :] == expert_iota)
    probs = route_scale * sig / jnp.sum(jnp.where(named, sig, 0.0), axis=0, keepdims=True)
    probs = jnp.where(named, probs, 0.0)
    rank = dot(mark(named), mark(iota((rows, rows), 0) < iota((rows, rows), 1)))
    base = (lax.rem(g, half_groups) * capacity).astype(f32)
    slots = jnp.where(named, base + rank, -1.0)
    kinds = 2 * local
    lanes = kinds * rows
    facts = jnp.concatenate([probs.astype(bf16), slots.astype(bf16)], axis=0)
    wide = dot(facts, mark(iota((rows, lanes), 1) % rows == iota((rows, lanes), 0)))
    line = iota((2 * experts, lanes), 0)
    kind = line // experts * local + line % local
    wide = jnp.where(kind == iota((2 * experts, lanes), 1) // rows, wide, 0.0).astype(bf16)
    owner = iota((groups, 2 * experts), 1) % experts // local
    notes = dot(mark(owner == iota((groups, 2 * experts), 0)), wide)
    for o in range(groups):
        notes_own[o] = notes[o : o + 1, :]
    pltpu.make_async_copy(notes_own.at[g], notes_all.at[g], note_recv).start()
    fetch[0].wait()
    pl.semaphore_wait(barrier, len(peers))
    for j in range(1, groups):
        note_copy(g, lax.rem(g + j, groups)).start()
    rows_copy(g, mate).start()
    for j in hops:
        rows_copy(g, flip(column, j) * 2 + side).start()

    order = [lax.rem(chip + 1 + i, chips) for i in range(chips)]
    partner = k + 1 - 2 * core

    def a_copy(b, i):
        if i == chips - 1:
            recv = kept_recv
        else:
            recv = a_recv.at[i, lax.rem(b, half_groups)]
        l = order[i]
        return remote(part.at[b, l], recv_a.at[b, l], a_send, recv, (g, partner))

    def multiply(*blocks):
        found = [block(b)[...] for b in blocks]
        found = found[0] if len(found) == 1 else jnp.concatenate(found, axis=0)
        for l in range(local):
            value = dot(found, w_ref[l]).astype(bf16)
            for i, b in enumerate(blocks):
                part[b, l] = value[i * rows : (i + 1) * rows]
        for i in range(chips):
            for b in blocks:
                pl.when(b // half_groups != core)(a_copy(b, i).start)

    def finish(b):
        at = lax.rem(b, half_groups)

        @pl.when(b // half_groups == core)
        def _():
            for i in range(chips - 1):
                l = order[i]
                a_copy(b, i).wait_recv()
                both = part[b, l].astype(f32) + recv_a[b, l].astype(f32)
                send_b[i, at] = both.astype(bf16)
                to = (g, l * 2 + core)
                remote(send_b.at[i, at], recv_b.at[chips - 2 - i, at], b_send, b_recv, to).start()

    eye = iota((rows, half_tokens), 0) == iota((rows, half_tokens), 1)

    slot = k * groups + g

    def score(b, home=False):
        for l in range(local):
            at = pl.ds(pl.multiple_of(b * rows, rows), rows)
            value = jnp.sum(
                saved_tok[l, at, :].astype(f32) * part[b, l].astype(f32), axis=1, keepdims=True
            )
            score_own[b, l : l + 1, :] = jnp.sum(
                jnp.where(eye, value, 0.0), axis=0, keepdims=True
            )
        if home:
            pltpu.make_async_copy(score_own.at[b], score_recv.at[slot], sc_recv).start()
        for dk in range(1 if home else 0, parts):
            to = (b, lax.rem(k + dk, parts))
            remote(score_own.at[b], score_recv.at[slot], sc_send, sc_recv, to).start()

    def tables():
        remote(notes_all, notes_all, note_send, note_recv, (g, k)).wait_recv()
        fetch[3].wait()
        diagonal = iota((rows, lanes), 1) % rows == iota((rows, lanes), 0)
        stack = [
            jnp.where(diagonal, jnp.broadcast_to(notes_all[b], (rows, lanes)), 0.0)
            for b in range(groups)
        ]
        stack = jnp.concatenate(stack, axis=0).astype(bf16)
        shape = (lanes, kinds * share)
        cols = dot(stack, mark(iota(shape, 0) // rows == iota(shape, 1) // share))
        spot = iota((tokens, share), 1).astype(f32)
        for l in range(local):
            weight = cols[:, l * share : (l + 1) * share]
            place = cols[:, (local + l) * share : (local + l + 1) * share]
            hit = place == spot
            match = mark(hit)
            scaled[l] = weight[:, 0:128]
            weight = jnp.where(hit, weight, 0.0).astype(bf16)
            for h in range(2):
                at = slice(h * half_tokens, (h + 1) * half_tokens)
                spread_ref[l, h] = weight[at]
                start = l * span + h * share
                saved_tok[l, at, :] = dot(
                    match[at], saved_ref[start : start + share, :]
                ).astype(bf16)

    near = [flip(column, j) * 2 + side for j in hops]
    far = [flip(column, j) * 2 + 1 - side for j in hops]
    w_copy.wait()
    multiply(g)
    rows_copy(mate, g).wait_recv()
    rows_copy(mate, near[-1]).start()
    multiply(mate)
    finish(g)
    tables()
    score(g, home=True)
    score(mate)
    for i, b in enumerate(near):
        rows_copy(b, g).wait_recv()
        if i < len(near) - 1:
            rows_copy(b, mate).start()
    multiply(*near)
    finish(mate)
    for b in near:
        score(b)
    for b in near:
        finish(b)
    last = None
    for b in [far[-1], *far[:-1]]:
        rows_copy(b, g).wait_recv()
        multiply(b)
        if last is not None:
            finish(last)
        score(b)
        last = b

    step = min(width, 256)

    def weigh(l):
        weighed = jnp.concatenate(
            [
                (scaled[l] * rows_all[:, n : n + 128].astype(f32)).astype(bf16)
                for n in range(0, features, 128)
            ],
            axis=1,
        )
        for n in range(0, width, step):
            weight_ref[l, :, n : n + step] = lax.dot_general(
                weighed, saved_tok[l, :, n : n + step], (((0,), (0,)), ((), ())),
                preferred_element_type=f32,
            ).astype(bf16)

    weigh(0)
    finish(last)
    for l in range(1, local):
        weigh(l)
    unit = mark(iota((share, share), 0) == iota((share, share), 1))
    spread = lax.dot_general(
        unit, spread_ref[chip, core], turn, preferred_element_type=f32
    ).astype(bf16)
    total = None
    held = pl.ds(core * half_groups, half_groups)
    whole = part.at[0:half_groups, 0]
    remote(whole, whole, a_send, kept_recv, (g, partner)).wait_recv()
    total = part[held, chip].astype(f32) + recv_a[held, chip].astype(f32)
    if chips > 1:
        arrived = recv_b.at[0 : chips - 1]
        remote(arrived, arrived, b_send, b_recv, (g, partner)).wait_recv()
    for i in range(chips - 1):
        total = total + recv_b[i].astype(f32)
    hidden_ref[...] = dot(spread, total.reshape(half_tokens, width).astype(bf16)).astype(bf16)

    remote(score_recv, score_recv, sc_send, sc_recv, (g, partner)).wait_recv()
    for o in range(groups):
        value = score_recv[o]
        for y in range(1, parts):
            value = value + score_recv[y * groups + o]
        score_rows[o * local : (o + 1) * local, :] = value
    pair = score_rows[:, 0:rows]
    mean = jnp.sum(probs * pair, axis=0, keepdims=True) / route_scale
    terms = jnp.where(named, probs * (1.0 - sig) * (pair - mean), 0.0).astype(bf16)
    turned = lax.dot_general(
        mark(iota((rows, rows), 0) == iota((rows, rows), 1)), terms, turn,
        preferred_element_type=f32,
    ).astype(bf16)
    fetch[4].wait()
    input_ref[...] = dot(turned, rw_ref[...]).astype(bf16)

    def sent(ref, sem):
        remote(ref, ref, sem, kept_recv, (g, partner)).wait_send()

    sent(rows_all.at[0 : (groups - 1) * rows, :], rows_send)
    sent(notes_all.at[0 : groups - 1], note_send)
    sent(part.at[0:half_groups], a_send)
    sent(send_b, b_send)
    sent(score_recv.at[0 : parts * groups - 1], sc_send)


def write_kernel(weight_ref, hidden_ref, input_ref, weight_hbm, hidden_hbm, input_hbm, sem):
    copies = [
        pltpu.make_async_copy(hidden_ref, hidden_hbm, sem.at[0]),
        pltpu.make_async_copy(input_ref, input_hbm, sem.at[1]),
    ]
    local, features, _ = weight_ref.shape
    cut = features // 4
    for l in range(local):
        for n in range(4):
            at = pl.ds(n * cut, cut)
            copies.append(
                pltpu.make_async_copy(
                    weight_ref.at[l, at, :], weight_hbm.at[l, at, :], sem.at[2 + l * 4 + n]
                )
            )
    for copy in copies:
        copy.start()
    for copy in copies:
        copy.wait()


def fused(out_grad, expert_ids, router_logits, router_weight, expert_weight, hidden_saved):
    groups, parts = lax.axis_size("grp"), lax.axis_size("ep")
    rows, features = out_grad.shape
    experts = router_logits.shape[1]
    top = expert_ids.shape[1]
    local, _, width = expert_weight.shape
    slots = hidden_saved.shape[1]
    span = slots // local
    half_groups = groups // 2
    half_tokens = half_groups * rows
    tokens = groups * rows
    share = span // 2
    chips = parts // 2
    f32, bf16 = jnp.float32, jnp.bfloat16
    vmem = pl.BlockSpec(memory_space=pltpu.VMEM)
    hbm = pl.BlockSpec(memory_space=pltpu.HBM)
    anyspace = pl.BlockSpec(memory_space=pl.ANY)
    dma = pltpu.SemaphoreType.DMA
    out_shape = (
        jax.ShapeDtypeStruct((local, features, width), bf16),
        jax.ShapeDtypeStruct((share, width), bf16),
        jax.ShapeDtypeStruct((rows, features), bf16),
    )
    pin = pltpu.with_memory_space_constraint
    outs = pl.pallas_call(
        fused_kernel,
        out_shape=tuple(pltpu.VMEM(x.shape, x.dtype) for x in out_shape),
        in_specs=[hbm] * 6,
        out_specs=(vmem, vmem, vmem),
        scratch_shapes=[
            pltpu.VMEM((top, rows), jnp.int32),
            pltpu.VMEM((experts, rows), f32),
            pltpu.VMEM((experts, features), bf16),
            pltpu.VMEM((local, features, width), bf16),
            pltpu.VMEM((slots, width), bf16),
            pltpu.VMEM((tokens, features), bf16),
            pltpu.VMEM((groups, 1, 2 * local * rows), f32),
            pltpu.VMEM((groups, 1, 2 * local * rows), f32),
            pltpu.VMEM((local, 2, half_tokens, share), bf16),
            pltpu.VMEM((local, tokens, width), bf16),
            pltpu.VMEM((local, tokens, 128), f32),
            pltpu.VMEM((groups, local, rows, width), bf16),
            pltpu.VMEM((groups, local, rows, width), bf16),
            pltpu.VMEM((chips - 1, half_groups, rows, width), bf16),
            pltpu.VMEM((chips - 1, half_groups, rows, width), bf16),
            pltpu.VMEM((groups, local, half_tokens), f32),
            pltpu.VMEM((parts * groups, local, half_tokens), f32),
            pltpu.VMEM((experts, half_tokens), f32),
            dma((5,)), dma, dma, dma((groups,)), dma, dma,
            dma, dma((chips - 1, half_groups)), dma, dma, dma, dma, dma,
        ],
        compiler_params=pltpu.CompilerParams(
            collective_id=0, has_side_effects=True, vmem_limit_bytes=40 * 1024 * 1024
        ),
    )(*[
        pin(x, pltpu.HBM)
        for x in (
            expert_ids.T, router_logits.T, out_grad, router_weight, expert_weight,
            hidden_saved.reshape(slots, width),
        )
    ])
    weight_grad, hidden, input_grad = pl.pallas_call(
        write_kernel,
        out_shape=out_shape,
        in_specs=[anyspace] * 3,
        out_specs=[hbm] * 3,
        scratch_shapes=[dma((2 + 4 * local,))],
        compiler_params=pltpu.CompilerParams(vmem_limit_bytes=16 * 1024 * 1024),
    )(*[pin(x, pltpu.VMEM) for x in outs])
    return weight_grad, hidden[None], input_grad


def choose(*args):
    out_grad, _, _, _, expert_weight, hidden_saved = args
    groups, parts = lax.axis_size("grp"), lax.axis_size("ep")
    rows, local = out_grad.shape[0], expert_weight.shape[0]
    slots_for_one = hidden_saved.shape[1] // groups
    lanes = groups // 2 * rows
    capacity = slots_for_one // local
    share = groups // 2 * capacity
    fits = rows <= capacity and lanes % 128 == 0 and share % 128 == 0 and share <= 256
    fits = fits and 2 * local * rows % 128 == 0 and groups & (groups - 1) == 0
    if parts == 2 * local and parts > 2 and groups % 2 == 0 and fits:
        return fused(*args)
    return body(*args)


def solution(mesh):
    in_specs = (
        P("grp", "ep"),
        P("grp", None),
        P("grp", None),
        P(None, "ep"),
        P("grp", "ep", None),
        P("grp", None, None),
    )
    out_specs = (P("grp", "ep", None), P("grp", "ep", None), P("grp", "ep"))
    return jax.shard_map(choose, mesh=mesh, in_specs=in_specs, out_specs=out_specs, check_vma=False)
```

```python
import jax
import jax.numpy as jnp
from jax import lax
from jax.experimental import pallas as pl
from jax.experimental.pallas import tpu as pltpu
from jax.sharding import PartitionSpec as P

route_scale = 2.5


def body(out_grad, expert_ids, router_logits, router_weight, expert_weight, hidden_saved):
    group_rows, features = out_grad.shape
    top_count = expert_ids.shape[1]
    experts = router_logits.shape[1]
    group_count = lax.axis_size("grp")
    local_experts = expert_weight.shape[0]
    hidden_width = expert_weight.shape[2]
    slot_count = hidden_saved.shape[1]
    capacity = slot_count // (local_experts * group_count)
    expert_span = group_count * capacity
    pair_count = group_rows * top_count
    sig_values = jax.nn.sigmoid(router_logits)
    picked = expert_ids[:, :, None] == jnp.arange(experts, dtype=jnp.int32)[None, None, :]
    chosen = jnp.sum(jnp.where(picked, sig_values[:, None, :], 0.0), axis=2)
    route_probs = route_scale * chosen / jnp.sum(chosen, axis=1, keepdims=True)
    flat_ids = expert_ids.reshape(pair_count)
    onehot = picked.reshape(pair_count, experts).astype(jnp.int32)
    pair_ranks = jnp.sum((jnp.cumsum(onehot, axis=0) - 1) * onehot, axis=1)
    slot_place = (
        flat_ids % local_experts * group_count + flat_ids // local_experts
    ) * capacity + pair_ranks
    slot_match = slot_place[None, :] == jnp.arange(slot_count, dtype=jnp.int32)[:, None]
    token_pick = jnp.sum(
        slot_match.reshape(slot_count, group_rows, top_count).astype(jnp.float32), axis=2
    ).astype(jnp.bfloat16)
    send_rows = jnp.dot(token_pick, out_grad, preferred_element_type=jnp.float32).astype(
        jnp.bfloat16
    )
    send_prob = jnp.sum(
        jnp.where(slot_match, route_probs.reshape(1, pair_count), 0.0), axis=1
    ).astype(jnp.bfloat16)
    got_rows, got_prob = (
        lax.all_to_all(
            send_rows.reshape(local_experts, group_count, capacity, features),
            "grp",
            split_axis=1,
            concat_axis=1,
            tiled=True,
        ),
        lax.all_to_all(
            send_prob.reshape(local_experts, group_count, capacity),
            "grp",
            split_axis=1,
            concat_axis=1,
            tiled=True,
        ),
    )
    slot_grads = got_rows.reshape(local_experts, expert_span, features)
    prob_rows = got_prob.reshape(local_experts, expert_span).astype(jnp.float32)
    saved_rows = hidden_saved.reshape(local_experts, expert_span, hidden_width)
    scaled_rows = (prob_rows[:, :, None] * slot_grads.astype(jnp.float32)).astype(jnp.bfloat16)
    weight_grad = jnp.einsum(
        "lmd,lmf->ldf", scaled_rows, saved_rows, preferred_element_type=jnp.float32
    ).astype(jnp.bfloat16)
    owner_index = lax.axis_index("ep")
    share_rows = slot_count // lax.axis_size("ep")
    flat_prob = prob_rows.reshape(slot_count)
    flat_saved = hidden_saved.reshape(slot_count, hidden_width)
    partial_term = jnp.einsum(
        "lmd,ldf->lmf", slot_grads, expert_weight, preferred_element_type=jnp.float32
    ).reshape(slot_count, hidden_width)
    rounded_term = lax.optimization_barrier(partial_term.astype(jnp.bfloat16)).astype(jnp.float32)
    partial_score = jnp.sum(flat_saved.astype(jnp.float32) * rounded_term, axis=1)
    moved_scores = lax.all_to_all(
        partial_score.reshape(local_experts, group_count, capacity),
        "grp",
        split_axis=1,
        concat_axis=1,
        tiled=True,
    )
    returned = lax.psum(moved_scores, "ep")
    summed = lax.psum_scatter(
        partial_term.astype(jnp.bfloat16), "ep", scatter_dimension=0, tiled=True
    ).astype(jnp.float32)
    own_prob = lax.dynamic_slice_in_dim(flat_prob, owner_index * share_rows, share_rows, 0)
    hidden_grad = (own_prob[:, None] * summed).astype(jnp.bfloat16)[None]
    pair_score = jnp.sum(
        jnp.where(slot_match, returned.reshape(slot_count, 1), 0.0), axis=0
    ).reshape(group_rows, top_count)
    weighted_mean = jnp.sum(route_probs * pair_score, axis=1, keepdims=True) / route_scale
    logit_terms = route_probs * (1.0 - chosen) * (pair_score - weighted_mean)
    router_grad = jnp.sum(jnp.where(picked, logit_terms[:, :, None], 0.0), axis=1).astype(
        jnp.bfloat16
    )
    input_grad = jnp.dot(router_grad, router_weight, preferred_element_type=jnp.float32).astype(
        jnp.bfloat16
    )
    return (weight_grad, hidden_grad, input_grad)


MESH = pl.DeviceIdType.MESH


def flip(a, j):
    out, bit = a, 1
    while bit <= j:
        if j & bit:
            out = out + bit * (1 - 2 * (a // bit % 2))
        bit *= 2
    return out


def fused_kernel(
    ids_hbm, logits_hbm, grad_hbm, rw_hbm, w_hbm, saved_hbm,
    weight_ref, total_out, spread_out, score_out, prob_out, gain_out, rw_ref,
    ids_ref, logits_ref, w_ref, saved_ref, rows_all, notes_own, notes_all,
    spread_ref, saved_tok, scaled, part, recv_a, send_b, recv_b,
    score_own, score_recv,
    in_sem, w_sem, rows_send, rows_recv, note_send, note_recv,
    a_send, a_recv, kept_recv, b_send, b_recv, sc_send, sc_recv,
):
    groups = lax.axis_size("grp")
    parts = lax.axis_size("ep")
    chips = parts // 2
    g = lax.axis_index("grp")
    k = lax.axis_index("ep")
    chip, core = k // 2, k % 2
    experts, rows = logits_ref.shape
    top = ids_ref.shape[0]
    _, local, _, width = part.shape
    features = rows_all.shape[1]
    half_groups = groups // 2
    half_tokens = half_groups * rows
    tokens = groups * rows
    span = saved_ref.shape[0] // local
    share = span // 2
    capacity = span // groups
    f32, bf16 = jnp.float32, jnp.bfloat16
    column, side = g // 2, lax.rem(g, 2)
    mate = g + 1 - 2 * side
    hops = list(range(half_groups - 1, 0, -1))
    turn = (((1,), (1,)), ((), ()))

    def iota(shape, dim):
        return lax.broadcasted_iota(jnp.int32, shape, dim)

    def mark(mask):
        return mask.astype(f32).astype(bf16)

    def dot(a, b):
        return jnp.dot(a, b, preferred_element_type=f32)

    barrier = pltpu.get_barrier_semaphore()
    peers = [(lax.rem(g + j, groups), k) for j in range(1, groups)]
    peers += [(g, lax.rem(k + j, parts)) for j in range(1, parts)]
    for peer in peers:
        pl.semaphore_signal(barrier, inc=1, device_id=peer, device_id_type=MESH)

    def block(b):
        return rows_all.at[pl.ds(pl.multiple_of(b * rows, rows), rows), :]

    fetch = [
        pltpu.make_async_copy(src, dst, in_sem.at[i])
        for i, (src, dst) in enumerate([
            (grad_hbm, block(g)), (logits_hbm, logits_ref), (ids_hbm, ids_ref),
            (saved_hbm, saved_ref), (rw_hbm, rw_ref),
        ])
    ]
    w_copy = pltpu.make_async_copy(w_hbm, w_ref, w_sem)
    for copy in [*fetch[1:3], fetch[0], w_copy, *fetch[3:]]:
        copy.start()

    def remote(src, dst, send, recv, to):
        return pltpu.make_async_remote_copy(
            src_ref=src, dst_ref=dst, send_sem=send, recv_sem=recv, device_id=to,
            device_id_type=MESH,
        )

    def rows_copy(b, to):
        data = block(b)
        return remote(data, data, rows_send, rows_recv.at[b], (to, k))

    def note_copy(b, to):
        return remote(notes_own.at[to], notes_all.at[b], note_send, note_recv, (to, k))

    fetch[1].wait()
    fetch[2].wait()
    sig = 1.0 / (1.0 + jnp.exp(-logits_ref[...]))
    ids = ids_ref[...]
    expert_iota = iota((experts, rows), 0)
    named = ids[0:1, :] == expert_iota
    for i in range(1, top):
        named = named | (ids[i : i + 1, :] == expert_iota)
    probs = route_scale * sig / jnp.sum(jnp.where(named, sig, 0.0), axis=0, keepdims=True)
    probs = jnp.where(named, probs, 0.0)
    rank = dot(mark(named), mark(iota((rows, rows), 0) < iota((rows, rows), 1)))
    base = (lax.rem(g, half_groups) * capacity).astype(f32)
    slots = jnp.where(named, base + rank, -1.0)
    kinds = 2 * local
    lanes = kinds * rows
    facts = jnp.concatenate([probs.astype(bf16), slots.astype(bf16)], axis=0)
    wide = dot(facts, mark(iota((rows, lanes), 1) % rows == iota((rows, lanes), 0)))
    line = iota((2 * experts, lanes), 0)
    kind = line // experts * local + line % local
    wide = jnp.where(kind == iota((2 * experts, lanes), 1) // rows, wide, 0.0).astype(bf16)
    owner = iota((groups, 2 * experts), 1) % experts // local
    notes = dot(mark(owner == iota((groups, 2 * experts), 0)), wide)
    for o in range(groups):
        notes_own[o] = notes[o : o + 1, :]
    pltpu.make_async_copy(notes_own.at[g], notes_all.at[g], note_recv).start()
    fetch[0].wait()
    pl.semaphore_wait(barrier, len(peers))
    for j in range(1, groups):
        note_copy(g, lax.rem(g + j, groups)).start()
    near = [flip(column, j) * 2 + side for j in hops]
    far = [flip(column, j) * 2 + 1 - side for j in hops]
    rows_copy(g, mate).start()
    for j, b in zip(hops, near):
        rows_copy(g, b).start()

    order = [lax.rem(chip + 1 + i, chips) for i in range(chips)]
    partner = k + 1 - 2 * core

    def a_copy(b, i):
        if i == chips - 1:
            recv = kept_recv
        else:
            recv = a_recv.at[i, lax.rem(b, half_groups)]
        l = order[i]
        return remote(part.at[b, l], recv_a.at[b, l], a_send, recv, (g, partner))

    def multiply(*blocks):
        found = [block(b)[...] for b in blocks]
        found = found[0] if len(found) == 1 else jnp.concatenate(found, axis=0)
        for l in range(local):
            value = dot(found, w_ref[l]).astype(bf16)
            for i, b in enumerate(blocks):
                part[b, l] = value[i * rows : (i + 1) * rows]
        for i in range(chips):
            for b in blocks:
                pl.when(b // half_groups != core)(a_copy(b, i).start)

    def finish(b):
        at = lax.rem(b, half_groups)

        @pl.when(b // half_groups == core)
        def _():
            for i in range(chips - 1):
                l = order[i]
                a_copy(b, i).wait_recv()
                both = part[b, l].astype(f32) + recv_a[b, l].astype(f32)
                send_b[i, at] = both.astype(bf16)
                to = (g, l * 2 + core)
                remote(send_b.at[i, at], recv_b.at[chips - 2 - i, at], b_send, b_recv, to).start()

    eye = iota((rows, half_tokens), 0) == iota((rows, half_tokens), 1)

    slot = k * groups + g

    def score(b, home=False):
        for l in range(local):
            at = pl.ds(pl.multiple_of(b * rows, rows), rows)
            value = jnp.sum(
                saved_tok[l, at, :].astype(f32) * part[b, l].astype(f32), axis=1, keepdims=True
            )
            score_own[b, l : l + 1, :] = jnp.sum(
                jnp.where(eye, value, 0.0), axis=0, keepdims=True
            )
        if home:
            pltpu.make_async_copy(score_own.at[b], score_recv.at[slot], sc_recv).start()
        for dk in range(1 if home else 0, parts):
            to = (b, lax.rem(k + dk, parts))
            remote(score_own.at[b], score_recv.at[slot], sc_send, sc_recv, to).start()

    def tables():
        remote(notes_all, notes_all, note_send, note_recv, (g, k)).wait_recv()
        fetch[3].wait()
        diagonal = iota((rows, lanes), 1) % rows == iota((rows, lanes), 0)
        stack = [
            jnp.where(diagonal, jnp.broadcast_to(notes_all[b], (rows, lanes)), 0.0)
            for b in range(groups)
        ]
        stack = jnp.concatenate(stack, axis=0).astype(bf16)
        shape = (lanes, kinds * share)
        cols = dot(stack, mark(iota(shape, 0) // rows == iota(shape, 1) // share))
        spot = iota((tokens, share), 1).astype(f32)
        for l in range(local):
            weight = cols[:, l * share : (l + 1) * share]
            place = cols[:, (local + l) * share : (local + l + 1) * share]
            hit = place == spot
            match = mark(hit)
            scaled[l] = weight[:, 0:128]
            weight = jnp.where(hit, weight, 0.0).astype(bf16)
            for h in range(2):
                at = slice(h * half_tokens, (h + 1) * half_tokens)
                spread_ref[l, h] = weight[at]
                start = l * span + h * share
                saved_tok[l, at, :] = dot(
                    match[at], saved_ref[start : start + share, :]
                ).astype(bf16)

    w_copy.wait()
    multiply(g)
    rows_copy(mate, g).wait_recv()
    rows_copy(mate, near[-1]).start()
    multiply(mate)
    finish(g)
    ahead = max(len(near) - 2, 0)
    tables()
    score(g, home=True)
    score(mate)
    finish(mate)
    for j, b in zip(hops, near):
        rows_copy(b, g).wait_recv()
        if j > 1:
            rows_copy(b, mate).start()
    multiply(*near)
    for b in near:
        score(b)
    first = [far[-1], *far[:ahead]]
    for b in first:
        rows_copy(b, g).wait_recv()
    multiply(*first)
    for b in first:
        score(b)
    for b in near:
        finish(b)
    last = far[ahead:-1]
    for b in last:
        rows_copy(b, g).wait_recv()
        multiply(b)
    for b in last:
        score(b)
    for b in first:
        finish(b)

    step = min(width, 256)

    def weigh(l):
        weighed = jnp.concatenate(
            [
                (scaled[l] * rows_all[:, n : n + 128].astype(f32)).astype(bf16)
                for n in range(0, features, 128)
            ],
            axis=1,
        )
        for n in range(0, width, step):
            weight_ref[l, :, n : n + step] = lax.dot_general(
                weighed, saved_tok[l, :, n : n + step], (((0,), (0,)), ((), ())),
                preferred_element_type=f32,
            ).astype(bf16)

    weigh(0)
    for b in last:
        finish(b)
    for l in range(1, local):
        weigh(l)
    unit = mark(iota((share, share), 0) == iota((share, share), 1))
    spread_out[...] = lax.dot_general(
        unit, spread_ref[chip, core], turn, preferred_element_type=f32
    ).astype(bf16)
    prob_out[...] = probs
    gain_out[...] = jnp.where(named, probs * (1.0 - sig), 0.0)
    fetch[4].wait()
    held = pl.ds(core * half_groups, half_groups)
    whole = part.at[0:half_groups, 0]
    remote(whole, whole, a_send, kept_recv, (g, partner)).wait_recv()
    total = part[held, chip].astype(f32) + recv_a[held, chip].astype(f32)
    if chips > 1:
        arrived = recv_b.at[0 : chips - 1]
        remote(arrived, arrived, b_send, b_recv, (g, partner)).wait_recv()
    for i in range(chips - 1):
        total = total + recv_b[i].astype(f32)
    total_out[...] = total.reshape(half_tokens, width).astype(bf16)
    remote(score_recv, score_recv, sc_send, sc_recv, (g, partner)).wait_recv()
    for o in range(groups):
        value = score_recv[o]
        for y in range(1, parts):
            value = value + score_recv[y * groups + o]
        score_out[o * local : (o + 1) * local, :] = value

    def sent(ref, sem):
        remote(ref, ref, sem, kept_recv, (g, partner)).wait_send()

    sent(rows_all.at[0 : (groups - 1) * rows, :], rows_send)
    sent(notes_all.at[0 : groups - 1], note_send)
    sent(part.at[0:half_groups], a_send)
    sent(send_b, b_send)
    sent(score_recv.at[0 : parts * groups - 1], sc_send)


def write_kernel(
    weight_ref, total_ref, spread_ref, score_ref, prob_ref, gain_ref, rw_ref,
    weight_hbm, hidden_hbm, input_hbm, hidden_ref, input_ref, sem,
):
    local = weight_ref.shape[0]
    rows = input_ref.shape[0]
    f32, bf16 = jnp.float32, jnp.bfloat16
    copies = [
        pltpu.make_async_copy(weight_ref.at[l], weight_hbm.at[l], sem.at[2 + l])
        for l in range(local)
    ]
    for copy in copies:
        copy.start()
    hidden_ref[...] = jnp.dot(
        spread_ref[...], total_ref[...], preferred_element_type=f32
    ).astype(bf16)
    copies.append(pltpu.make_async_copy(hidden_ref, hidden_hbm, sem.at[0]))
    copies[-1].start()
    pair = score_ref[:, 0:rows]
    mean = jnp.sum(prob_ref[...] * pair, axis=0, keepdims=True) / route_scale
    terms = (gain_ref[...] * (pair - mean)).astype(bf16)
    eye = lax.broadcasted_iota(jnp.int32, (rows, rows), 0) == lax.broadcasted_iota(
        jnp.int32, (rows, rows), 1
    )
    turned = lax.dot_general(
        eye.astype(f32).astype(bf16), terms, (((1,), (1,)), ((), ())),
        preferred_element_type=f32,
    ).astype(bf16)
    input_ref[...] = jnp.dot(turned, rw_ref[...], preferred_element_type=f32).astype(bf16)
    copies.append(pltpu.make_async_copy(input_ref, input_hbm, sem.at[1]))
    copies[-1].start()
    for copy in copies:
        copy.wait()


def fused(out_grad, expert_ids, router_logits, router_weight, expert_weight, hidden_saved):
    groups, parts = lax.axis_size("grp"), lax.axis_size("ep")
    rows, features = out_grad.shape
    experts = router_logits.shape[1]
    top = expert_ids.shape[1]
    local, _, width = expert_weight.shape
    slots = hidden_saved.shape[1]
    span = slots // local
    half_groups = groups // 2
    half_tokens = half_groups * rows
    tokens = groups * rows
    share = span // 2
    chips = parts // 2
    f32, bf16 = jnp.float32, jnp.bfloat16
    vmem = pl.BlockSpec(memory_space=pltpu.VMEM)
    hbm = pl.BlockSpec(memory_space=pltpu.HBM)
    anyspace = pl.BlockSpec(memory_space=pl.ANY)
    dma = pltpu.SemaphoreType.DMA
    out_shape = (
        jax.ShapeDtypeStruct((local, features, width), bf16),
        jax.ShapeDtypeStruct((share, width), bf16),
        jax.ShapeDtypeStruct((rows, features), bf16),
    )
    pin = pltpu.with_memory_space_constraint
    outs = pl.pallas_call(
        fused_kernel,
        out_shape=(
            pltpu.VMEM((local, features, width), bf16),
            pltpu.VMEM((share, width), bf16),
            pltpu.VMEM((share, half_tokens), bf16),
            pltpu.VMEM((experts, half_tokens), f32),
            pltpu.VMEM((experts, rows), f32),
            pltpu.VMEM((experts, rows), f32),
            pltpu.VMEM((experts, features), bf16),
        ),
        in_specs=[hbm] * 6,
        out_specs=(vmem,) * 7,
        scratch_shapes=[
            pltpu.VMEM((top, rows), jnp.int32),
            pltpu.VMEM((experts, rows), f32),
            pltpu.VMEM((local, features, width), bf16),
            pltpu.VMEM((slots, width), bf16),
            pltpu.VMEM((tokens, features), bf16),
            pltpu.VMEM((groups, 1, 2 * local * rows), f32),
            pltpu.VMEM((groups, 1, 2 * local * rows), f32),
            pltpu.VMEM((local, 2, half_tokens, share), bf16),
            pltpu.VMEM((local, tokens, width), bf16),
            pltpu.VMEM((local, tokens, 128), f32),
            pltpu.VMEM((groups, local, rows, width), bf16),
            pltpu.VMEM((groups, local, rows, width), bf16),
            pltpu.VMEM((chips - 1, half_groups, rows, width), bf16),
            pltpu.VMEM((chips - 1, half_groups, rows, width), bf16),
            pltpu.VMEM((groups, local, half_tokens), f32),
            pltpu.VMEM((parts * groups, local, half_tokens), f32),
            dma((5,)), dma, dma, dma((groups,)), dma, dma,
            dma, dma((chips - 1, half_groups)), dma, dma, dma, dma, dma,
        ],
        compiler_params=pltpu.CompilerParams(
            collective_id=0, has_side_effects=True, vmem_limit_bytes=40 * 1024 * 1024
        ),
    )(*[
        pin(x, pltpu.HBM)
        for x in (
            expert_ids.T, router_logits.T, out_grad, router_weight, expert_weight,
            hidden_saved.reshape(slots, width),
        )
    ])
    weight_grad, hidden, input_grad = pl.pallas_call(
        write_kernel,
        out_shape=out_shape,
        in_specs=[anyspace, *[vmem] * 6],
        out_specs=[hbm] * 3,
        scratch_shapes=[
            pltpu.VMEM((share, width), bf16), pltpu.VMEM((rows, features), bf16),
            dma((2 + local,)),
        ],
        compiler_params=pltpu.CompilerParams(vmem_limit_bytes=16 * 1024 * 1024),
    )(*[pin(x, pltpu.VMEM) for x in outs])
    return weight_grad, hidden[None], input_grad


def choose(*args):
    out_grad, _, _, _, expert_weight, hidden_saved = args
    groups, parts = lax.axis_size("grp"), lax.axis_size("ep")
    rows, local = out_grad.shape[0], expert_weight.shape[0]
    slots_for_one = hidden_saved.shape[1] // groups
    lanes = groups // 2 * rows
    capacity = slots_for_one // local
    share = groups // 2 * capacity
    fits = rows <= capacity and lanes % 128 == 0 and share % 128 == 0 and share <= 256
    fits = fits and 2 * local * rows % 128 == 0 and groups & (groups - 1) == 0
    if parts == 2 * local and parts > 2 and groups > 2 and fits:
        return fused(*args)
    return body(*args)


def solution(mesh):
    in_specs = (
        P("grp", "ep"),
        P("grp", None),
        P("grp", None),
        P(None, "ep"),
        P("grp", "ep", None),
        P("grp", None, None),
    )
    out_specs = (P("grp", "ep", None), P("grp", "ep", None), P("grp", "ep"))
    return jax.shard_map(choose, mesh=mesh, in_specs=in_specs, out_specs=out_specs, check_vma=False)
```
